32 devices in a mesh: slab: 8 (over y, x, core), det: 4 (over z).
Axes of the slice: x: 2, y: 2, z: 4, core: 2. Of those that a mesh axis runs over, the one named last changes fastest.
Arguments:
- traces: float32 [32, 128, 4096], P(('slab', 'det')), may hold values from -6 to 6
- tables: bfloat16 [32, 256, 2048], P('slab', None, 'det'), may hold values from -0.0625 to 0.0625
- slab_range: int32 [32, 2], P(('slab', 'det')), may hold values from 0 to 7, as said below
- table_slot: int32 [32, 7], P(('slab', 'det')), may hold values from 0 to 3
- sample_start: int32 [32, 7], P(('slab', 'det')), may hold values from 0 to 3840
Outputs:
- image: float32 [128, 16384], P(None, ('slab', 'det'))
The draws below stay inside these ranges and needn't reach their ends.
Inputs may be any that keep to these rules, and one draw needn't show every extreme that they name: For detector d with home slab g = d // 4: max(0, g - 3) <= slab_range[d, 0] <= g <= slab_range[d, 1] <= min(7, g + 3); some detectors reach the full 3 on both sides where the grid allows.
All inputs are finite; a program needn't handle non-finite values.
Results may differ from the reference program's by a relative error of at most 0.007.
Values may be sent and summed in bfloat16 or wider, within the bound.
A program may use at most 64 MiB of HBM per device.

```python
import jax
import jax.numpy as jnp
from jax import lax

SAMP = 4096
KWIN = 256
NTAB = 4
RANGE = 3
VOX = 2048
FRAMES = 128
DET_DEV = 1
DETS = 32
N_SLAB = 8
N_DET = 4


def draw_slab_range(key, part):
    lower_key, upper_key = jax.random.split(jax.random.fold_in(key, 11))
    detector_index = jnp.arange(DETS, dtype=jnp.int32)
    home = detector_index // (N_DET * DET_DEV)
    lower_reach = jax.random.randint(lower_key, (DETS,), 0, RANGE + 1)
    upper_reach = jax.random.randint(upper_key, (DETS,), 0, RANGE + 1)
    widest = detector_index % 7 == 0
    lower_reach = jnp.where(widest, RANGE, lower_reach)
    upper_reach = jnp.where(widest, RANGE, upper_reach)
    first_slab = jnp.maximum(home - lower_reach, 0)
    last_slab = jnp.minimum(home + upper_reach, N_SLAB - 1)
    return jnp.stack([first_slab, last_slab], axis=1).astype(jnp.int32)


def plant(entries, rng, smallest, largest):
    longest = entries.shape.index(max(entries.shape))
    spots = []
    for shift in (0, 1):
        where = [jax.random.randint(jax.random.fold_in(rng, axis), (), 0, length) for axis, length in enumerate(entries.shape)]
        where[longest] = (where[longest] + shift) % entries.shape[longest]
        spots.append(tuple(where))
    return entries.at[spots[0]].set(smallest).at[spots[1]].set(largest)


def block_levels(key, shape, cuts, smallest, top_value):
    def one(dim, parts):
        steps = jax.random.uniform(jax.random.fold_in(jax.random.fold_in(key, 6), dim), (parts,), jnp.float32, smallest / len(cuts), top_value / len(cuts))
        return jnp.repeat(jnp.exp(steps), shape[dim] // parts).reshape((-1,) + (1,) * (len(shape) - dim - 1))

    loudness = one(*cuts[0])
    for cut in cuts[1:]:
        loudness = loudness * one(*cut)
    return loudness


def normal_values(key, shape, deviation, bound, cuts=(), kind=jnp.bfloat16):
    array = jax.random.normal(key, shape, jnp.float32) * deviation
    if len(cuts) > 0:
        array = block_levels(key, shape, cuts, -0.22, 0.18) * array
    return jnp.clip(array, min=-bound, max=bound).astype(kind)


def setup_inputs(seed: int = 0) -> dict:
    splits = jax.random.split(jax.random.key(seed), 6)
    traces = normal_values(splits[0], (DETS, FRAMES, SAMP), 1.0, 6.0, ((0, 32),), jnp.float32)
    tables = normal_values(splits[1], (N_SLAB * NTAB, KWIN, N_SLAB * 0 + VOX), (4 * (2 * RANGE + 1) * DET_DEV * KWIN) ** -0.5, 0.0625, ((0, 8), (2, 4)))
    slab_range = draw_slab_range(jax.random.fold_in(splits[5], 71), 0)
    table_slot = plant(jax.random.randint(splits[3], (DETS, 2 * RANGE + 1), 0, NTAB), jax.random.fold_in(splits[3], 1), 0, NTAB - 1).astype(jnp.int32)
    sample_start = plant(jax.random.randint(splits[4], (DETS, 2 * RANGE + 1), 0, SAMP - KWIN + 1), jax.random.fold_in(splits[4], 1), 0, SAMP - KWIN).astype(jnp.int32)
    return {"traces": traces, "tables": tables, "slab_range": slab_range, "table_slot": table_slot, "sample_start": sample_start}


def windows_for(trace_rows, starts):
    def single(trace_row, first_index):
        return lax.dynamic_slice_in_dim(trace_row, first_index, KWIN, 1)
    return jax.vmap(single)(trace_rows, starts)


def reference(traces, tables, slab_range, table_slot, sample_start):
    group = N_DET * DET_DEV
    table_blocks = tables.reshape(N_SLAB, NTAB, KWIN, VOX)
    slot_values = jnp.arange(NTAB, dtype=jnp.int32)

    def one_slab(slab):
        stacked = jnp.zeros((N_DET, NTAB, FRAMES, KWIN), jnp.float32)
        for offset in range(-RANGE, RANGE + 1):
            home = slab - offset
            valid = (home >= 0) & (home < N_SLAB)
            clipped = jnp.clip(home, 0, N_SLAB - 1)
            first_row = (clipped * group).astype(jnp.int32)
            trace_rows = lax.dynamic_slice_in_dim(traces, first_row, group, 0).astype(jnp.bfloat16)
            ranges = lax.dynamic_slice_in_dim(slab_range, first_row, group, 0)
            slot_ids = lax.dynamic_slice_in_dim(table_slot, first_row, group, 0)[:, offset + RANGE]
            starts = lax.dynamic_slice_in_dim(sample_start, first_row, group, 0)[:, offset + RANGE]
            active = valid & (ranges[:, 0] <= slab) & (slab <= ranges[:, 1])
            windows = windows_for(trace_rows, starts).astype(jnp.float32)
            windows = windows.reshape(N_DET, DET_DEV, FRAMES, KWIN)
            onehot = ((slot_ids[:, None] == slot_values[None, :]) & active[:, None]).astype(jnp.float32)
            onehot = onehot.reshape(N_DET, DET_DEV, NTAB)
            stacked = stacked + jnp.einsum("kit,kifw->ktfw", onehot, windows)
        rounded = stacked.astype(jnp.bfloat16).astype(jnp.float32)
        weights = table_blocks[slab].astype(jnp.float32)
        return jnp.einsum("ktfw,twv->fv", rounded, weights)

    slabs = lax.map(one_slab, jnp.arange(N_SLAB, dtype=jnp.int32))
    return jnp.transpose(slabs, (1, 0, 2)).reshape(FRAMES, N_SLAB * VOX)
```

```python
import functools

import jax
import jax.numpy as jnp
from jax import lax
from jax.experimental import pallas as pl
from jax.experimental.pallas import tpu as pltpu
from jax.sharding import PartitionSpec as P

MESH = pl.DeviceIdType.MESH
KWIN = 256
NTAB = 4
RANGE = 3
LANES = 128
OFFSETS = 2 * RANGE + 1
ROWS = 16
LAG = 4
WORK = jnp.float32
BITS = (1, 2, 4, 8, 16, 32, 64)
AWAY = [o for o in range(OFFSETS) if o != RANGE]


def kernel(
    n_slab, n_det,
    traces, tables, slab_range, table_slot, sample_start, out,
    table_buf, range_buf, slot_buf, start_buf,
    send_win, got_win, send_mask, got_mask,
    own, up, from_outer, from_inner, down,
    trace_sem, table_sem, small_sem,
    win_send, win_recv, mask_send, mask_recv,
    up_send, outer_recv, down_send, inner_recv,
    *trace_bufs,
):
    slab, det = lax.axis_index("slab"), lax.axis_index("det")
    n_chunk = send_win.shape[0]
    half = n_det // 2

    smalls = [
        pltpu.make_async_copy(src, dst, small_sem.at[i])
        for i, (src, dst) in enumerate(
            [(sample_start, start_buf), (slab_range, range_buf), (table_slot, slot_buf)]
        )
    ]
    for copy in smalls:
        copy.start()

    def rows_of(c):
        return pl.ds(c * ROWS, ROWS)

    loads = [
        pltpu.make_async_copy(traces.at[0, rows_of(c)], trace_bufs[c], trace_sem.at[c])
        for c in range(n_chunk)
    ]
    for copy in loads:
        copy.start()
    table_load = pltpu.make_async_copy(tables, table_buf, table_sem)
    table_load.start()

    def valid(to):
        return (to >= 0) & (to < n_slab)

    left = det < half
    inner = jnp.where(left, det + 1, det - 1)
    outer = jnp.where(left, det - 1, det + 1)

    barrier = pltpu.get_barrier_semaphore()
    peers = jnp.int32(0)
    for o in AWAY:
        peer = slab + (o - RANGE)
        peers = peers + valid(peer).astype(jnp.int32)

        @pl.when(valid(peer))
        def _():
            pl.semaphore_signal(barrier, 1, device_id=(peer, det), device_id_type=MESH)

    for step in (-1, 1):
        near = det + step
        there = (near >= 0) & (near < n_det)
        peers = peers + there.astype(jnp.int32)

        @pl.when(there)
        def _():
            pl.semaphore_signal(barrier, 1, device_id=(slab, near), device_id_type=MESH)

    for o in AWAY:

        @pl.when(jnp.logical_not(valid(slab - (o - RANGE))))
        def _():
            got_mask[o] = jnp.zeros(got_mask.shape[1:], got_mask.dtype)
            for c in range(n_chunk):
                got_win[c, o] = jnp.zeros(got_win.shape[2:], got_win.dtype)

    def mask_copy(o):
        return pltpu.make_async_remote_copy(
            src_ref=send_mask.at[o], dst_ref=got_mask.at[o],
            send_sem=mask_send.at[o], recv_sem=mask_recv.at[o],
            device_id=(slab + (o - RANGE), det), device_id_type=MESH,
        )

    def win_copy(c, o):
        return pltpu.make_async_remote_copy(
            src_ref=send_win.at[c, o], dst_ref=got_win.at[c, o],
            send_sem=win_send.at[c, o], recv_sem=win_recv.at[c, o],
            device_id=(slab + (o - RANGE), det), device_id_type=MESH,
        )

    def up_copy(c, cross):
        return pltpu.make_async_remote_copy(
            src_ref=up.at[c], dst_ref=(from_inner if cross else from_outer).at[c],
            send_sem=up_send.at[c], recv_sem=(inner_recv if cross else outer_recv).at[c],
            device_id=(slab, inner), device_id_type=MESH,
        )

    def down_copy(c):
        return pltpu.make_async_remote_copy(
            src_ref=down.at[c], dst_ref=from_inner.at[c],
            send_sem=down_send.at[c], recv_sem=inner_recv.at[c],
            device_id=(slab, outer), device_id_type=MESH,
        )

    for copy in smalls:
        copy.wait()
    n_tile = traces.shape[2] // LANES
    steps = [1 << b for b in reversed(range((n_tile - 1).bit_length()))]
    lane = lax.broadcasted_iota(jnp.int32, (ROWS, LANES), 1)
    mask_rows = lax.broadcasted_iota(jnp.int32, send_mask.shape[1:], 0)
    hits, turns, keeps = [], [], []
    for o in range(OFFSETS):
        target = slab + (o - RANGE)
        low, high, slot = (
            jnp.full(mask_rows.shape, value)
            for value in (range_buf[0, 0], range_buf[0, 1], slot_buf[0, o])
        )
        hit = (low <= target) & (target <= high) & (mask_rows == slot)
        send_mask[o] = hit.astype(jnp.float32)
        start = jnp.full(lane.shape, start_buf[0, o])
        hits.append([(start & (step * LANES)) != 0 for step in steps])
        turns.append([(start & bit) != 0 for bit in BITS])
        keeps.append(lane < LANES - (start & (LANES - 1)))

    def window(c, o):
        def tile(i):
            i = min(i, n_tile - 1)
            return trace_bufs[c][:, i * LANES : (i + 1) * LANES].astype(WORK)

        tiles = None
        for step, hit in zip(steps, hits[o]):
            get = tile if tiles is None else tiles.__getitem__
            tiles = [jnp.where(hit, get(i + step), get(i)) for i in range(step + 2)]
        for bit, hit in zip(BITS, turns[o]):
            tiles = [jnp.where(hit, pltpu.roll(x, LANES - bit, 1), x) for x in tiles]
        for i in range(KWIN // LANES):
            piece = jnp.where(keeps[o], tiles[i], tiles[i + 1])
            send_win[c, o, :, i * LANES : (i + 1) * LANES] = piece.astype(jnp.bfloat16)

    for c in range(n_chunk):
        loads[c].wait()
        for o in range(OFFSETS):
            window(c, o)
        if c == 0:
            pl.semaphore_wait(barrier, peers)
        for o in AWAY:

            @pl.when(valid(slab + (o - RANGE)))
            def _():
                if c == 0:
                    mask_copy(o).start()
                win_copy(c, o).start()

    def stack(c):
        for o in AWAY:

            @pl.when(valid(slab - (o - RANGE)))
            def _():
                if c == 0:
                    mask_copy(o).wait_recv()
                win_copy(c, o).wait_recv()

        bins = [jnp.zeros((ROWS, KWIN), jnp.float32) for _ in range(NTAB)]
        for o in range(OFFSETS):
            if o == RANGE:
                win, mask = send_win[c, o], send_mask
            else:
                win, mask = got_win[c, o], got_mask
            win = win.astype(jnp.float32)
            for t in range(NTAB):
                weight = jnp.concatenate([mask[o, t : t + 1]] * (KWIN // LANES), axis=1)
                bins[t] = bins[t] + weight * win
        return bins

    def cols(t):
        return slice(t * KWIN, (t + 1) * KWIN)

    def weights():
        return table_buf[...].reshape(NTAB * KWIN, table_buf.shape[2])

    def image(ref, c, n):
        sums = ref[c : c + n].reshape(n * ROWS, NTAB * KWIN)
        out[c * ROWS : (c + n) * ROWS] = jnp.dot(
            sums, weights(), preferred_element_type=jnp.float32
        )

    def role(has_outer, cross):
        def send_up(c):
            bins = stack(c)
            if has_outer:
                up_copy(c, False).wait_recv()
            for t in range(NTAB):
                total = bins[t]
                if has_outer:
                    total = total + from_outer[c, :, cols(t)].astype(jnp.float32)
                if cross:
                    own[c, :, cols(t)] = total
                up[c, :, cols(t)] = total.astype(jnp.bfloat16)
            up_copy(c, cross).start()

        def send_down(c):
            down_copy(c).wait_recv()
            if cross:
                for t in range(NTAB):
                    total = own[c, :, cols(t)] + from_inner[c, :, cols(t)].astype(jnp.float32)
                    down[c, :, cols(t)] = total.astype(jnp.bfloat16)
            else:
                down[c] = from_inner[c]
            down_copy(c).start()

        if has_outer or cross:
            for i in range(n_chunk + LAG):
                if i < n_chunk:
                    send_up(i)
                if i >= LAG:
                    send_down(i - LAG)
            table_load.wait()
            image(down, 0, n_chunk)
        else:
            for c in range(n_chunk):
                send_up(c)
            table_load.wait()
            pair = 2
            for c in range(n_chunk):
                down_copy(c).wait_recv()
                if c % pair == pair - 1:
                    image(from_inner, c + 1 - pair, pair)
        for c in range(n_chunk):
            up_copy(c, cross).wait_send()
            if has_outer:
                down_copy(c).wait_send()

    edge = (det == 0) | (det == n_det - 1)
    pl.when(edge)(lambda: role(False, False))
    pl.when(jnp.logical_not(edge))(lambda: role(True, True))

    for o in AWAY:

        @pl.when(valid(slab + (o - RANGE)))
        def _():
            mask_copy(o).wait_send()
            for c in range(n_chunk):
                win_copy(c, o).wait_send()


def body(n_slab, n_det, traces, tables, slab_range, table_slot, sample_start):
    _, frames, samp = traces.shape
    voxels = tables.shape[2]
    n_chunk = frames // ROWS
    wide = NTAB * KWIN
    mask_rows = -(-NTAB // 8) * 8
    anywhere = pl.BlockSpec(memory_space=pl.ANY)
    dma = pltpu.SemaphoreType.DMA
    return pl.pallas_call(
        functools.partial(kernel, n_slab, n_det),
        out_shape=pltpu.VMEM((frames, voxels), jnp.float32),
        in_specs=[anywhere] * 5,
        out_specs=pl.BlockSpec(memory_space=pltpu.VMEM),
        scratch_shapes=[
            pltpu.VMEM(tables.shape, jnp.bfloat16),
            pltpu.SMEM(slab_range.shape, jnp.int32),
            pltpu.SMEM(table_slot.shape, jnp.int32),
            pltpu.SMEM(sample_start.shape, jnp.int32),
            pltpu.VMEM((n_chunk, OFFSETS, ROWS, KWIN), jnp.bfloat16),
            pltpu.VMEM((n_chunk, OFFSETS, ROWS, KWIN), jnp.bfloat16),
            pltpu.VMEM((OFFSETS, mask_rows, LANES), jnp.float32),
            pltpu.VMEM((OFFSETS, mask_rows, LANES), jnp.float32),
            pltpu.VMEM((n_chunk, ROWS, wide), jnp.float32),
            pltpu.VMEM((n_chunk, ROWS, wide), jnp.bfloat16),
            pltpu.VMEM((n_chunk, ROWS, wide), jnp.bfloat16),
            pltpu.VMEM((n_chunk, ROWS, wide), jnp.bfloat16),
            pltpu.VMEM((n_chunk, ROWS, wide), jnp.bfloat16),
            dma((n_chunk,)),
            dma,
            dma((3,)),
            dma((n_chunk, OFFSETS)),
            dma((n_chunk, OFFSETS)),
            dma((OFFSETS,)),
            dma((OFFSETS,)),
            dma((n_chunk,)),
            dma((n_chunk,)),
            dma((n_chunk,)),
            dma((n_chunk,)),
            *[pltpu.VMEM((ROWS, samp), jnp.float32) for _ in range(n_chunk)],
        ],
        compiler_params=pltpu.CompilerParams(
            collective_id=0, has_side_effects=True, vmem_limit_bytes=66_500_000
        ),
    )(traces, tables, slab_range, table_slot, sample_start)


def solution(mesh):
    placed = (
        P(("slab", "det"), None, None),
        P("slab", None, "det"),
        P(("slab", "det"), None),
        P(("slab", "det"), None),
        P(("slab", "det"), None),
    )
    return jax.shard_map(
        functools.partial(body, mesh.shape["slab"], mesh.shape["det"]),
        mesh=mesh, in_specs=placed, out_specs=P(None, ("slab", "det")), check_vma=False,
    )
```

```python
import functools

import jax
import jax.numpy as jnp
from jax import lax
from jax.experimental import pallas as pl
from jax.experimental.pallas import tpu as pltpu
from jax.sharding import PartitionSpec as P

MESH = pl.DeviceIdType.MESH
KWIN = 256
NTAB = 4
RANGE = 3
LANES = 128
SUBLANES = 8
OFFSETS = 2 * RANGE + 1
ROWS = 16
LAG = 4
AWAY = [o for o in range(OFFSETS) if o != RANGE]


def kernel(
    n_slab, n_det,
    traces, tables, slab_range, table_slot, sample_start, out,
    table_buf, range_buf, slot_buf, start_buf,
    send_win, got_win, send_mask, got_mask,
    own, up, from_outer, from_inner, down,
    trace_sem, table_sem, small_sem,
    win_send, win_recv, mask_send, mask_recv,
    up_send, outer_recv, down_send, inner_recv,
    *trace_bufs,
):
    slab, det = lax.axis_index("slab"), lax.axis_index("det")
    n_chunk = got_win.shape[0]
    half = n_det // 2

    smalls = [
        pltpu.make_async_copy(src, dst, small_sem.at[i])
        for i, (src, dst) in enumerate(
            [(sample_start, start_buf), (slab_range, range_buf), (table_slot, slot_buf)]
        )
    ]
    for copy in smalls:
        copy.start()
    groups = ROWS // SUBLANES
    loads = [
        pltpu.make_async_copy(
            traces.at[pl.ds(c * groups, groups)], trace_bufs[c], trace_sem.at[c]
        )
        for c in range(n_chunk)
    ]
    for copy in loads:
        copy.start()
    table_load = pltpu.make_async_copy(tables, table_buf, table_sem)
    table_load.start()

    def valid(to):
        return (to >= 0) & (to < n_slab)

    left = det < half
    inner = jnp.where(left, det + 1, det - 1)
    outer = jnp.where(left, det - 1, det + 1)

    barrier = pltpu.get_barrier_semaphore()
    partners = jnp.int32(0)
    for o in AWAY:
        peer = slab + (o - RANGE)
        partners = partners + valid(peer).astype(jnp.int32)

        @pl.when(valid(peer))
        def _():
            pl.semaphore_signal(barrier, 1, device_id=(peer, det), device_id_type=MESH)

    peers = partners
    for step in (-1, 1):
        near = det + step
        there = (near >= 0) & (near < n_det)
        peers = peers + there.astype(jnp.int32)

        @pl.when(there)
        def _():
            pl.semaphore_signal(barrier, 1, device_id=(slab, near), device_id_type=MESH)

    for o in AWAY:

        @pl.when(jnp.logical_not(valid(slab - (o - RANGE))))
        def _():
            got_mask[o] = jnp.zeros(got_mask.shape[1:], got_mask.dtype)
            for c in range(n_chunk):
                got_win[c, o] = jnp.zeros(got_win.shape[2:], got_win.dtype)

    def mask_copy(o, n=None):
        at = o if n is None else pl.ds(o, n)
        return pltpu.make_async_remote_copy(
            src_ref=send_mask.at[at], dst_ref=got_mask.at[at],
            send_sem=mask_send, recv_sem=mask_recv,
            device_id=(slab + (o - RANGE), det), device_id_type=MESH,
        )

    def win_copy(c, o):
        return pltpu.make_async_remote_copy(
            src_ref=send_win.at[o, c], dst_ref=got_win.at[c, o],
            send_sem=win_send.at[o], recv_sem=win_recv.at[c],
            device_id=(slab + (o - RANGE), det), device_id_type=MESH,
        )

    def up_copy(c, cross):
        return pltpu.make_async_remote_copy(
            src_ref=up.at[c], dst_ref=(from_inner if cross else from_outer).at[c],
            send_sem=up_send, recv_sem=(inner_recv if cross else outer_recv).at[c],
            device_id=(slab, inner), device_id_type=MESH,
        )

    def down_copy(c):
        return pltpu.make_async_remote_copy(
            src_ref=down.at[c], dst_ref=from_inner.at[c],
            send_sem=down_send, recv_sem=inner_recv.at[c],
            device_id=(slab, outer), device_id_type=MESH,
        )

    def per_partners(wait):
        for n in range(1, OFFSETS):
            pl.when(partners == n)(functools.partial(wait, n))

    for copy in smalls:
        copy.wait()
    n_tile = traces.shape[1]
    lane = lax.broadcasted_iota(jnp.int32, (SUBLANES, LANES), 1)
    mask_rows = lax.broadcasted_iota(jnp.int32, send_mask.shape[1:], 0)
    firsts, backs, keeps = [], [], []
    for o in range(OFFSETS):
        target = slab + (o - RANGE)
        low, high, slot = (
            jnp.full(mask_rows.shape, value)
            for value in (range_buf[0, 0], range_buf[0, 1], slot_buf[0, o])
        )
        hit = (low <= target) & (target <= high) & (mask_rows == slot)
        send_mask[o] = hit.astype(jnp.float32)
        start = start_buf[0, o]
        firsts.append(start >> 7)
        past = start & (LANES - 1)
        backs.append((LANES - past) & (LANES - 1))
        keeps.append(lane < LANES - past)

    def window(c, o):
        for i in range(KWIN // LANES):
            pieces = []
            for g in range(groups):
                x, y = (
                    pltpu.roll(
                        trace_bufs[c][g, jnp.minimum(firsts[o] + i + k, n_tile - 1)], backs[o], 1
                    )
                    for k in range(2)
                )
                pieces.append(jnp.where(keeps[o], x, y))
            piece = jnp.concatenate(pieces, axis=0).astype(jnp.bfloat16)
            send_win[o, c, :, i * LANES : (i + 1) * LANES] = piece

    def send(c, parity):
        for o in AWAY:
            to = slab + (o - RANGE)

            @pl.when(valid(to) & (lax.rem(slab + (o + OFFSETS), 2) == parity))
            def _():
                if c == 0:
                    mask_copy(o).start()
                win_copy(c, o).start()

    for c in range(n_chunk):
        loads[c].wait()
        for o in range(OFFSETS):
            window(c, o)
        if c == 0:
            pl.semaphore_wait(barrier, peers)
        send(c, 0)
    for c in range(n_chunk):
        send(c, 1)

    def stack(c):
        @per_partners
        def _(n):
            if c == 0:
                mask_copy(0, n).wait_recv()
            pltpu.make_async_copy(
                got_win.at[c, pl.ds(0, n)], got_win.at[c, pl.ds(0, n)], win_recv.at[c]
            ).wait()

        bins = [jnp.zeros((ROWS, KWIN), jnp.float32) for _ in range(NTAB)]
        for o in range(OFFSETS):
            if o == RANGE:
                win, mask = send_win[o, c], send_mask
            else:
                win, mask = got_win[c, o], got_mask
            win = win.astype(jnp.float32)
            for t in range(NTAB):
                weight = jnp.concatenate([mask[o, t : t + 1]] * (KWIN // LANES), axis=1)
                bins[t] = bins[t] + weight * win
        return bins

    def cols(t):
        return slice(t * KWIN, (t + 1) * KWIN)

    def weights():
        return table_buf[...].reshape(NTAB * KWIN, table_buf.shape[2])

    def image(ref, c, n):
        sums = ref[c : c + n].reshape(n * ROWS, NTAB * KWIN)
        out[c * ROWS : (c + n) * ROWS] = jnp.dot(
            sums, weights(), preferred_element_type=jnp.float32
        )

    def role(has_outer, cross):
        def send_up(c):
            bins = stack(c)
            if has_outer:
                up_copy(c, False).wait_recv()
            for t in range(NTAB):
                total = bins[t]
                if has_outer:
                    total = total + from_outer[c, :, cols(t)].astype(jnp.float32)
                if cross:
                    own[c, :, cols(t)] = total
                up[c, :, cols(t)] = total.astype(jnp.bfloat16)
            up_copy(c, cross).start()

        def send_down(c):
            down_copy(c).wait_recv()
            if cross:
                for t in range(NTAB):
                    total = own[c, :, cols(t)] + from_inner[c, :, cols(t)].astype(jnp.float32)
                    down[c, :, cols(t)] = total.astype(jnp.bfloat16)
            else:
                down[c] = from_inner[c]
            down_copy(c).start()

        if has_outer or cross:
            for i in range(n_chunk + LAG):
                if i < n_chunk:
                    send_up(i)
                if i >= LAG:
                    send_down(i - LAG)
            table_load.wait()
            image(down, 0, n_chunk)
        else:
            for c in range(n_chunk):
                send_up(c)
            table_load.wait()
            pair = 2
            for c in range(n_chunk):
                down_copy(c).wait_recv()
                if c % pair == pair - 1:
                    image(from_inner, c + 1 - pair, pair)
        for used, copied, sem in ((True, up, up_send), (has_outer, down, down_send)):
            if used:
                pltpu.make_async_copy(copied, copied, sem).wait()

    edge = (det == 0) | (det == n_det - 1)
    pl.when(edge)(lambda: role(False, False))
    pl.when(jnp.logical_not(edge))(lambda: role(True, True))

    @per_partners
    def _(n):
        mask_copy(0, n).wait_send()

    for o in AWAY:

        @pl.when(valid(slab + (o - RANGE)))
        def _():
            pltpu.make_async_copy(send_win.at[o], send_win.at[o], win_send.at[o]).wait()


def body(n_slab, n_det, traces, tables, slab_range, table_slot, sample_start):
    _, frames, samp = traces.shape
    voxels = tables.shape[2]
    n_chunk = frames // ROWS
    n_tile = samp // LANES
    tiled = traces.reshape(frames // SUBLANES, SUBLANES, n_tile, LANES).transpose(0, 2, 1, 3)
    wide = NTAB * KWIN
    mask_rows = -(-NTAB // 8) * 8
    anywhere = pl.BlockSpec(memory_space=pl.ANY)
    dma = pltpu.SemaphoreType.DMA
    return pl.pallas_call(
        functools.partial(kernel, n_slab, n_det),
        out_shape=pltpu.VMEM((frames, voxels), jnp.float32),
        in_specs=[anywhere] * 5,
        out_specs=pl.BlockSpec(memory_space=pltpu.VMEM),
        scratch_shapes=[
            pltpu.VMEM(tables.shape, jnp.bfloat16),
            pltpu.SMEM(slab_range.shape, jnp.int32),
            pltpu.SMEM(table_slot.shape, jnp.int32),
            pltpu.SMEM(sample_start.shape, jnp.int32),
            pltpu.VMEM((OFFSETS, n_chunk, ROWS, KWIN), jnp.bfloat16),
            pltpu.VMEM((n_chunk, OFFSETS, ROWS, KWIN), jnp.bfloat16),
            pltpu.VMEM((OFFSETS, mask_rows, LANES), jnp.float32),
            pltpu.VMEM((OFFSETS, mask_rows, LANES), jnp.float32),
            pltpu.VMEM((n_chunk, ROWS, wide), jnp.float32),
            pltpu.VMEM((n_chunk, ROWS, wide), jnp.bfloat16),
            pltpu.VMEM((n_chunk, ROWS, wide), jnp.bfloat16),
            pltpu.VMEM((n_chunk, ROWS, wide), jnp.bfloat16),
            pltpu.VMEM((n_chunk, ROWS, wide), jnp.bfloat16),
            dma((n_chunk,)),
            dma,
            dma((3,)),
            dma((OFFSETS,)),
            dma((n_chunk,)),
            dma,
            dma,
            dma,
            dma((n_chunk,)),
            dma,
            dma((n_chunk,)),
            *[
                pltpu.VMEM((ROWS // SUBLANES, n_tile, SUBLANES, LANES), jnp.float32)
                for _ in range(n_chunk)
            ],
        ],
        compiler_params=pltpu.CompilerParams(
            collective_id=0, has_side_effects=True, vmem_limit_bytes=66_500_000
        ),
    )(tiled, tables, slab_range, table_slot, sample_start)


def solution(mesh):
    placed = (
        P(("slab", "det"), None, None),
        P("slab", None, "det"),
        P(("slab", "det"), None),
        P(("slab", "det"), None),
        P(("slab", "det"), None),
    )
    return jax.shard_map(
        functools.partial(body, mesh.shape["slab"], mesh.shape["det"]),
        mesh=mesh, in_specs=placed, out_specs=P(None, ("slab", "det")), check_vma=False,
    )
```

```python
import functools

import jax
import jax.numpy as jnp
from jax import lax
from jax.experimental import pallas as pl
from jax.experimental.pallas import tpu as pltpu
from jax.sharding import PartitionSpec as P

MESH = pl.DeviceIdType.MESH
KWIN = 256
NTAB = 4
RANGE = 3
LANES = 128
SUBLANES = 8
OFFSETS = 2 * RANGE + 1
ROWS = 16
LAG = 4
DIRECT = 3
LEAD = 3
GROUP = 2
AWAY = [o for o in range(OFFSETS) if o != RANGE]


def n_far_of(n_det, n_chunk):
    return min(DIRECT, n_chunk) if n_det > 3 else 0


def kernel(
    n_slab, n_det,
    traces, tables, slab_range, table_slot, sample_start, out,
    table_buf, range_buf, slot_buf, start_buf,
    send_win, got_win, far_win, send_mask, got_mask, far_mask,
    own, up, from_outer, from_inner, down,
    trace_sem, table_sem, small_sem,
    win_send, win_recv, far_recv, mask_send, mask_recv, far_mask_send, far_mask_recv,
    up_send, outer_recv, down_send, inner_recv,
    *trace_bufs,
):
    slab, det = lax.axis_index("slab"), lax.axis_index("det")
    n_chunk = got_win.shape[0]
    n_far = n_far_of(n_det, n_chunk)
    half = max(n_det // 2, 1)

    smalls = [
        pltpu.make_async_copy(src, dst, small_sem.at[i])
        for i, (src, dst) in enumerate(
            [(sample_start, start_buf), (slab_range, range_buf), (table_slot, slot_buf)]
        )
    ]
    for copy in smalls:
        copy.start()
    groups = ROWS // SUBLANES
    loads = [
        pltpu.make_async_copy(
            traces.at[pl.ds(c * groups, groups)], trace_bufs[c], trace_sem.at[c]
        )
        for c in range(n_chunk)
    ]
    for copy in loads:
        copy.start()
    table_load = pltpu.make_async_copy(tables, table_buf, table_sem)
    table_load.start()

    def valid(to):
        return (to >= 0) & (to < n_slab)

    left = det < half
    inner = jnp.where(left, det + 1, det - 1)
    outer = jnp.where(left, det - 1, det + 1)

    barrier = pltpu.get_barrier_semaphore()
    partners = jnp.int32(0)
    for o in AWAY:
        peer = slab + (o - RANGE)
        partners = partners + valid(peer).astype(jnp.int32)

        @pl.when(valid(peer))
        def _():
            pl.semaphore_signal(barrier, 1, device_id=(peer, det), device_id_type=MESH)

    edge = (det == 0) | (det == n_det - 1)
    beside = (det == 1) | (det == n_det - 2)
    peers = partners
    if n_far:
        peers = peers + jnp.where(edge, partners, 0)
        for o in AWAY:
            peer = slab + (o - RANGE)

            @pl.when(valid(peer) & beside)
            def _():
                pl.semaphore_signal(barrier, 1, device_id=(peer, outer), device_id_type=MESH)

    for step in (-1, 1):
        near = det + step
        there = (near >= 0) & (near < n_det)
        told = there
        heard = there
        if n_far:
            told = there & jnp.logical_not(edge)
            heard = there & (near > 0) & (near < n_det - 1)
        peers = peers + heard.astype(jnp.int32)

        @pl.when(told)
        def _():
            pl.semaphore_signal(barrier, 1, device_id=(slab, near), device_id_type=MESH)

    for o in AWAY:

        @pl.when(jnp.logical_not(valid(slab - (o - RANGE))))
        def _():
            got_mask[o] = jnp.full(got_mask.shape[1:], -1, got_mask.dtype)
            if n_far:
                far_mask[o] = jnp.full(far_mask.shape[1:], -1, far_mask.dtype)
            for c in range(n_far):
                far_win[c, o] = jnp.zeros(far_win.shape[2:], far_win.dtype)
            for c in range(n_chunk):
                got_win[c, o] = jnp.zeros(got_win.shape[2:], got_win.dtype)

    def mask_copy(o, n=None):
        at = o if n is None else pl.ds(o, n)
        return pltpu.make_async_remote_copy(
            src_ref=send_mask.at[at], dst_ref=got_mask.at[at],
            send_sem=mask_send, recv_sem=mask_recv,
            device_id=(slab + (o - RANGE), det), device_id_type=MESH,
        )

    def win_copy(c, o):
        return pltpu.make_async_remote_copy(
            src_ref=send_win.at[o, c], dst_ref=got_win.at[c, o],
            send_sem=win_send.at[o], recv_sem=win_recv.at[c],
            device_id=(slab + (o - RANGE), det), device_id_type=MESH,
        )

    def far_mask_copy(o, n=None):
        at = o if n is None else pl.ds(o, n)
        return pltpu.make_async_remote_copy(
            src_ref=send_mask.at[at], dst_ref=far_mask.at[at],
            send_sem=far_mask_send, recv_sem=far_mask_recv,
            device_id=(slab + (o - RANGE), inner), device_id_type=MESH,
        )

    def far_copy(c, o):
        return pltpu.make_async_remote_copy(
            src_ref=send_win.at[o, c], dst_ref=far_win.at[c, o],
            send_sem=win_send.at[o], recv_sem=far_recv.at[c],
            device_id=(slab + (o - RANGE), inner), device_id_type=MESH,
        )

    def up_copy(c, cross):
        return pltpu.make_async_remote_copy(
            src_ref=up.at[c], dst_ref=(from_inner if cross else from_outer).at[c],
            send_sem=up_send, recv_sem=(inner_recv if cross else outer_recv).at[c],
            device_id=(slab, inner), device_id_type=MESH,
        )

    def down_copy(c):
        return pltpu.make_async_remote_copy(
            src_ref=down.at[c], dst_ref=from_inner.at[c],
            send_sem=down_send, recv_sem=inner_recv.at[c],
            device_id=(slab, outer), device_id_type=MESH,
        )

    def per_partners(wait):
        for n in range(0, OFFSETS):
            pl.when(partners == n)(functools.partial(wait, n))

    for copy in smalls:
        copy.wait()
    n_tile = traces.shape[1]
    lane = lax.broadcasted_iota(jnp.int32, (SUBLANES, LANES), 1)
    firsts, backs, keeps = [], [], []
    for o in range(OFFSETS):
        target = slab + (o - RANGE)
        low, high, slot = (
            jnp.full(send_mask.shape[1:], value)
            for value in (range_buf[0, 0], range_buf[0, 1], slot_buf[0, o])
        )
        hit = (low <= target) & (target <= high)
        send_mask[o] = jnp.where(hit, slot, -1).astype(jnp.float32)
        start = start_buf[0, o]
        firsts.append(start >> 7)
        past = start & (LANES - 1)
        backs.append((LANES - past) & (LANES - 1))
        keeps.append(lane < LANES - past)

    def window(c, o):
        for i in range(KWIN // LANES):
            pieces = []
            for g in range(groups):
                x, y = (
                    pltpu.roll(
                        trace_bufs[c][g, jnp.minimum(firsts[o] + i + k, n_tile - 1)], backs[o], 1
                    )
                    for k in range(2)
                )
                pieces.append(jnp.where(keeps[o], x, y))
            piece = jnp.concatenate(pieces, axis=0).astype(jnp.bfloat16)
            send_win[o, c, :, i * LANES : (i + 1) * LANES] = piece

    def send(c, parity):
        for o in range(OFFSETS):
            to = slab + (o - RANGE)
            now = valid(to) & (lax.rem(slab + (o + OFFSETS), 2) == parity)
            if c < n_far:

                @pl.when(now & edge)
                def _():
                    if c == 0:
                        far_mask_copy(o).start()
                    far_copy(c, o).start()

            if o != RANGE:

                @pl.when(now & jnp.logical_not(edge) if c < n_far else now)
                def _():
                    win_copy(c, o).start()

                if c == 0:
                    pl.when(now)(lambda: mask_copy(o).start())

    for step in range(n_chunk + LEAD):
        if step < n_chunk:
            loads[step].wait()
            for o in range(OFFSETS):
                window(step, o)
            if step == 0:
                pl.semaphore_wait(barrier, peers)
            send(step, 0)
        if step >= LEAD:
            send(step - LEAD, 1)

    def stack(c, far):
        wins, masks, sem = (far_win, far_mask, far_recv) if far else (got_win, got_mask, win_recv)

        @per_partners
        def _(n):
            n = n + 1 if far else n
            if n:
                arrived = wins.at[c, pl.ds(0, n)]
                pltpu.make_async_copy(arrived, arrived, sem.at[c]).wait()

        bins = [jnp.zeros((ROWS, KWIN), jnp.float32) for _ in range(NTAB)]
        for o in range(OFFSETS):
            if o == RANGE and not far:
                win, mask = send_win[o, c], send_mask
            else:
                win, mask = wins[c, o], masks
            win = win.astype(jnp.float32)
            slot = jnp.concatenate([jnp.broadcast_to(mask[o], (ROWS, LANES))] * (KWIN // LANES), axis=1)
            for t in range(NTAB):
                bins[t] = bins[t] + jnp.where(slot == t, win, 0.0)
        return bins

    def wait_masks(far):
        @per_partners
        def _(n):
            if far:
                far_mask_copy(0, n + 1).wait_recv()
            elif n:
                mask_copy(0, n).wait_recv()

    def cols(t):
        return slice(t * KWIN, (t + 1) * KWIN)

    def weights():
        return table_buf[...].reshape(NTAB * KWIN, table_buf.shape[2])

    def image(ref, c, n):
        sums = ref[c : c + n].reshape(n * ROWS, NTAB * KWIN)
        out[c * ROWS : (c + n) * ROWS] = jnp.dot(
            sums, weights(), preferred_element_type=jnp.float32
        )

    def wait_sends(far):
        @per_partners
        def _(n):
            if n:
                mask_copy(0, n).wait_send()
            if far:
                far_mask_copy(0, n + 1).wait_send()

        for o in AWAY:

            @pl.when(valid(slab + (o - RANGE)))
            def _():
                pltpu.make_async_copy(send_win.at[o], send_win.at[o], win_send.at[o]).wait()

        if far:
            sent = send_win.at[RANGE, pl.ds(0, n_far)]
            pltpu.make_async_copy(sent, sent, win_send.at[RANGE]).wait()

    def role(has_outer, cross, gets_far):
        gives_far = n_far > 0 and not has_outer

        def send_up(c):
            far = gets_far and c < n_far
            bins = stack(c, False)
            if far:
                bins = [x + y for x, y in zip(bins, stack(c, True))]
            elif has_outer:
                up_copy(c, False).wait_recv()
            for t in range(NTAB):
                total = bins[t]
                if has_outer and not far:
                    total = total + from_outer[c, :, cols(t)].astype(jnp.float32)
                if cross:
                    own[c, :, cols(t)] = total
                up[c, :, cols(t)] = total.astype(jnp.bfloat16)
            up_copy(c, cross).start()

        def send_down(c):
            down_copy(c).wait_recv()
            if cross:
                for t in range(NTAB):
                    total = own[c, :, cols(t)] + from_inner[c, :, cols(t)].astype(jnp.float32)
                    down[c, :, cols(t)] = total.astype(jnp.bfloat16)
            else:
                down[c] = from_inner[c]
            if has_outer:
                down_copy(c).start()

        wait_masks(False)
        if gets_far:
            wait_masks(True)
        if has_outer or cross:
            for i in range(n_chunk + LAG):
                if i < n_chunk:
                    send_up(i)
                if i >= LAG:
                    send_down(i - LAG)
            table_load.wait()
            image(down, 0, n_chunk)
        else:
            first = n_far if gives_far else 0
            for c in range(first, n_chunk):
                send_up(c)
            wait_sends(gives_far)
            if first < n_chunk:
                sent = up.at[pl.ds(first, n_chunk - first)]
                pltpu.make_async_copy(sent, sent, up_send).wait()
            table_load.wait()
            for c in range(n_chunk):
                down_copy(c).wait_recv()
                if (c + 1) % GROUP == 0:
                    image(from_inner, c + 1 - GROUP, GROUP)
        if has_outer or cross:
            wait_sends(False)
            pltpu.make_async_copy(up, up, up_send).wait()
            if has_outer:
                pltpu.make_async_copy(down, down, down_send).wait()

    roles = {}
    for d in range(n_det):
        kind = (0 < d < n_det - 1, d in (half - 1, half), n_far > 0 and d in (1, n_det - 2))
        roles.setdefault(kind, []).append(d)
    for kind, members in roles.items():
        here = functools.reduce(jnp.logical_or, [det == d for d in members])
        pl.when(here)(functools.partial(role, *kind))


def body(n_slab, n_det, traces, tables, slab_range, table_slot, sample_start):
    _, frames, samp = traces.shape
    voxels = tables.shape[2]
    n_chunk = frames // ROWS
    n_far = n_far_of(n_det, n_chunk)
    n_tile = samp // LANES
    tiled = traces.reshape(frames // SUBLANES, SUBLANES, n_tile, LANES).transpose(0, 2, 1, 3)
    wide = NTAB * KWIN
    anywhere = pl.BlockSpec(memory_space=pl.ANY)
    dma = pltpu.SemaphoreType.DMA
    return pl.pallas_call(
        functools.partial(kernel, n_slab, n_det),
        out_shape=pltpu.VMEM((frames, voxels), jnp.float32),
        in_specs=[anywhere] * 5,
        out_specs=pl.BlockSpec(memory_space=pltpu.VMEM),
        scratch_shapes=[
            pltpu.VMEM(tables.shape, jnp.bfloat16),
            pltpu.SMEM(slab_range.shape, jnp.int32),
            pltpu.SMEM(table_slot.shape, jnp.int32),
            pltpu.SMEM(sample_start.shape, jnp.int32),
            pltpu.VMEM((OFFSETS, n_chunk, ROWS, KWIN), jnp.bfloat16),
            pltpu.VMEM((n_chunk, OFFSETS, ROWS, KWIN), jnp.bfloat16),
            pltpu.VMEM((max(n_far, 1), OFFSETS, ROWS, KWIN), jnp.bfloat16),
            pltpu.VMEM((OFFSETS, 1, LANES), jnp.float32),
            pltpu.VMEM((OFFSETS, 1, LANES), jnp.float32),
            pltpu.VMEM((OFFSETS, 1, LANES), jnp.float32),
            pltpu.VMEM((n_chunk, ROWS, wide), jnp.float32),
            pltpu.VMEM((n_chunk, ROWS, wide), jnp.bfloat16),
            pltpu.VMEM((n_chunk, ROWS, wide), jnp.bfloat16),
            pltpu.VMEM((n_chunk, ROWS, wide), jnp.bfloat16),
            pltpu.VMEM((n_chunk, ROWS, wide), jnp.bfloat16),
            dma((n_chunk,)),
            dma,
            dma((3,)),
            dma((OFFSETS,)),
            dma((n_chunk,)),
            dma((max(n_far, 1),)),
            dma,
            dma,
            dma,
            dma,
            dma,
            dma((n_chunk,)),
            dma,
            dma((n_chunk,)),
            *[
                pltpu.VMEM((ROWS // SUBLANES, n_tile, SUBLANES, LANES), jnp.float32)
                for _ in range(n_chunk)
            ],
        ],
        compiler_params=pltpu.CompilerParams(
            collective_id=0, has_side_effects=True, vmem_limit_bytes=66_500_000
        ),
    )(tiled, tables, slab_range, table_slot, sample_start)


def solution(mesh):
    placed = (
        P(("slab", "det"), None, None),
        P("slab", None, "det"),
        P(("slab", "det"), None),
        P(("slab", "det"), None),
        P(("slab", "det"), None),
    )
    return jax.shard_map(
        functools.partial(body, mesh.shape["slab"], mesh.shape["det"]),
        mesh=mesh, in_specs=placed, out_specs=P(None, ("slab", "det")), check_vma=False,
    )
```

```python
import functools

import jax
import jax.numpy as jnp
from jax import lax
from jax.experimental import pallas as pl
from jax.experimental.pallas import tpu as pltpu
from jax.sharding import PartitionSpec as P

MESH = pl.DeviceIdType.MESH
KWIN = 256
NTAB = 4
RANGE = 3
LANES = 128
SUBLANES = 8
OFFSETS = 2 * RANGE + 1
ROWS = 16
LAG = 7
DIRECT = 3
LEAD = 0
GROUP = 2
GROUPS = ROWS // SUBLANES


def sizes(n_slab, n_det, frames):
    pair = 2 if n_slab % 2 == 0 else 1
    n_chunk = frames // ROWS
    return pair, n_chunk, min(DIRECT, n_chunk) if n_det == 4 else 0


def kernel(
    n_slab, n_det,
    traces, tables, slab_range, table_slot, sample_start, out,
    first_buf, rest_buf, table_buf, range_buf, slot_buf, start_buf,
    send_win, got_win, far_win, send_mask, got_mask, far_mask,
    own, up, from_outer, from_inner, down,
    trace_sem, table_sem, small_sem,
    win_send, far_send, win_recv, mask_send, mask_recv, far_mask_send, far_mask_recv,
    up_send, outer_recv, down_send, client_send, inner_recv,
):
    slab, det = lax.axis_index("slab"), lax.axis_index("det")
    pair, n_chunk, n_far = sizes(n_slab, n_det, out.shape[0])
    half = n_det // 2

    smalls = [
        pltpu.make_async_copy(src, dst, small_sem.at[i])
        for i, (src, dst) in enumerate(
            [(sample_start, start_buf), (slab_range, range_buf), (table_slot, slot_buf)]
        )
    ]
    for copy in smalls:
        copy.start()
    loads = [
        pltpu.make_async_copy(traces.at[pl.ds(0, GROUPS)], first_buf, trace_sem.at[0]),
        pltpu.make_async_copy(
            traces.at[pl.ds(GROUPS, rest_buf.shape[0])], rest_buf, trace_sem.at[1]
        ),
    ]
    for copy in loads:
        copy.start()

    def valid(to):
        return (to >= 0) & (to < n_slab)

    def place(to):
        return lax.rem(to + pair * OFFSETS, pair)

    def hosts(to):
        return place(to) == pair - 1

    is_host = hosts(slab)
    host = slab - place(slab) + (pair - 1)
    left = det < half
    inner = jnp.where(left, det + 1, det - 1)
    outer = jnp.where(left, det - 1, det + 1)
    edge = (det == 0) | (det == n_det - 1)
    middle = (det == half - 1) | (det == half)

    def member(p):
        return host - (pair - 1) + p

    def sources(to):
        return jnp.minimum(to, RANGE) + jnp.minimum(n_slab - 1 - to, RANGE)

    source_counts = sorted({min(t, RANGE) + min(n_slab - 1 - t, RANGE) for t in range(n_slab)})

    def per_count(count, options, act):
        for n in options:
            pl.when(count == n)(functools.partial(act, n))

    barrier = pltpu.get_barrier_semaphore()
    heard = jnp.int32(0)

    def tell(condition, to, at):
        @pl.when(condition)
        def _():
            pl.semaphore_signal(barrier, 1, device_id=(to, at), device_id_type=MESH)

    for k in range(-RANGE, RANGE + pair):
        source, target = slab - k, slab + k
        writes = valid(target) & hosts(target)
        if k:
            tell(is_host & valid(source), source, det)
            heard = heard + writes.astype(jnp.int32)
        if n_far:
            tell(is_host & middle & valid(source), source, outer)
            heard = heard + (writes & edge).astype(jnp.int32)
    if n_far:
        tell(is_host & middle, slab, inner)
        heard = heard + (is_host & middle).astype(jnp.int32)
    else:
        for step in (-1, 1):
            near = det + step
            there = (near >= 0) & (near < n_det)
            for p in range(pair):
                tell(there & (is_host | (p == pair - 1)), member(p), near)
            heard = heard + jnp.where(there, jnp.where(is_host, pair, 1), 0)

    table_load = pltpu.make_async_copy(tables, table_buf, table_sem)
    table_load.start()

    for p in range(pair):
        for o in range(OFFSETS):

            @pl.when(is_host & jnp.logical_not(valid(member(p) - (o - RANGE))))
            def _():
                got_mask[p, o] = jnp.full(got_mask.shape[2:], -1, got_mask.dtype)
                far_mask[p, o] = jnp.full(far_mask.shape[2:], -1, far_mask.dtype)
                for c in range(n_chunk):
                    got_win[c, p, o] = jnp.zeros(got_win.shape[3:], got_win.dtype)
                for c in range(n_far):
                    far_win[c, p, o] = jnp.zeros(far_win.shape[3:], far_win.dtype)

    def send_copy(src, dst, to, at, sent, landed):
        return pltpu.make_async_remote_copy(
            src_ref=src, dst_ref=dst, send_sem=sent, recv_sem=landed,
            device_id=(to, at), device_id_type=MESH,
        )

    def await_bytes(ref, sem):
        pltpu.make_async_copy(ref, ref, sem).wait()

    def up_copy(c, p, cross):
        into, landed = (from_inner, inner_recv) if cross else (from_outer, outer_recv)
        return send_copy(up.at[c, p], into.at[c, p], slab, inner, up_send, landed.at[c, p])

    def down_copy(c, p):
        return send_copy(
            down.at[c, p], from_inner.at[c, p], member(p), outer, down_send, inner_recv.at[c, p]
        )

    def client_copy(c, p):
        return send_copy(
            down.at[c, p], from_inner.at[c, p], member(p), det, client_send, inner_recv.at[c, p]
        )

    for copy in smalls:
        copy.wait()
    n_tile = traces.shape[1]
    lane = lax.broadcasted_iota(jnp.int32, (SUBLANES, LANES), 1)
    firsts, backs, keeps = [], [], []
    for o in range(OFFSETS):
        target = slab + (o - RANGE)
        low, high, slot = (
            jnp.full(send_mask.shape[1:], value)
            for value in (range_buf[0, 0], range_buf[0, 1], slot_buf[0, o])
        )
        hit = (low <= target) & (target <= high)
        send_mask[o] = jnp.where(hit, slot, -1).astype(jnp.float32)
        start = start_buf[0, o]
        firsts.append(start >> 7)
        past = start & (LANES - 1)
        backs.append((LANES - past) & (LANES - 1))
        keeps.append(lane < LANES - past)

    def window(c, o):
        buf, base = (first_buf, 0) if c == 0 else (rest_buf, (c - 1) * GROUPS)
        for i in range(KWIN // LANES):
            pieces = []
            for g in range(GROUPS):
                x, y = (
                    pltpu.roll(
                        buf[base + g, jnp.minimum(firsts[o] + i + k, n_tile - 1)], backs[o], 1
                    )
                    for k in range(2)
                )
                pieces.append(jnp.where(keeps[o], x, y))
            piece = jnp.concatenate(pieces, axis=0).astype(jnp.bfloat16)
            send_win[o, c, :, i * LANES : (i + 1) * LANES] = piece

    def send(c, p):
        for o in range(OFFSETS):
            to = slab + (o - RANGE)
            at = to - p + (pair - 1)
            now = valid(to) & (place(to) == p)
            away = now & (at != slab)
            if c < n_far:

                @pl.when(now & edge)
                def _():
                    if c == 0:
                        send_copy(
                            send_mask.at[o], far_mask.at[p, o], at, inner,
                            far_mask_send, far_mask_recv.at[p],
                        ).start()
                    send_copy(
                        send_win.at[o, c], far_win.at[c, p, o], at, inner,
                        far_send, outer_recv.at[c, p],
                    ).start()

            @pl.when(away & jnp.logical_not(edge) if c < n_far else away)
            def _():
                send_copy(
                    send_win.at[o, c], got_win.at[c, p, o], at, det, win_send, win_recv.at[c, p]
                ).start()

            if c == 0:

                @pl.when(away)
                def _():
                    send_copy(
                        send_mask.at[o], got_mask.at[p, o], at, det, mask_send, mask_recv.at[p]
                    ).start()

    for step in range(n_chunk + LEAD):
        if step < n_chunk:
            if step < len(loads):
                loads[step].wait()
            for o in range(OFFSETS):
                window(step, o)
            if step == 0:
                pl.semaphore_wait(barrier, heard)
            send(step, 0)
        if step >= LEAD:
            for p in range(1, pair):
                send(step - LEAD, p)

    def stack(c, p, far):
        wins, masks, sem = (
            (far_win, far_mask, outer_recv) if far else (got_win, got_mask, win_recv)
        )

        def arrive(n):
            n = n + 1 if far else n
            if n:
                arrived = wins.at[c, p, pl.ds(0, n)]
                await_bytes(arrived, sem.at[c, p])

        per_count(sources(member(p)), source_counts, arrive)
        mine = None if far else RANGE - (pair - 1) + p
        bins = [jnp.zeros((ROWS, KWIN), jnp.float32) for _ in range(NTAB)]
        for o in range(OFFSETS):
            if o == mine:
                win, mask = send_win[o, c], send_mask[o]
            else:
                win, mask = wins[c, p, o], masks[p, o]
            win = win.astype(jnp.float32)
            slot = jnp.broadcast_to(mask, (ROWS, LANES))
            slot = jnp.concatenate([slot] * (KWIN // LANES), axis=1)
            for t in range(NTAB):
                bins[t] = bins[t] + jnp.where(slot == t, win, 0.0)
        return bins

    def wait_masks(masks, sem, extra):
        for p in range(pair):

            def arrive(n):
                if n + extra:
                    await_bytes(masks.at[p, pl.ds(0, n + extra)], sem.at[p])

            per_count(sources(member(p)), source_counts, arrive)

    def cols(t):
        return slice(t * KWIN, (t + 1) * KWIN)

    def image(ref, p, c, n):
        sums = ref[c : c + n, p].reshape(n * ROWS, NTAB * KWIN)
        weights = table_buf[...].reshape(NTAB * KWIN, table_buf.shape[2])
        out[c * ROWS : (c + n) * ROWS] = jnp.dot(
            sums, weights, preferred_element_type=jnp.float32
        )

    def wait_sends(hosting, far):
        local = pair if hosting else 0

        def sent(n):
            n = n + 1
            if n > local:
                chunks = pl.ds(far, n_chunk - far)
                if far < n_chunk:
                    await_bytes(send_win.at[pl.ds(0, n - local), chunks], win_send)
                await_bytes(send_mask.at[pl.ds(0, n - local)], mask_send)
            if far:
                await_bytes(send_win.at[pl.ds(0, n), pl.ds(0, far)], far_send)
                await_bytes(send_mask.at[pl.ds(0, n)], far_mask_send)

        per_count(sources(slab), source_counts, sent)

    def finish(p):
        table_load.wait()
        for c in range(n_chunk):
            await_bytes(from_inner.at[c, p], inner_recv.at[c, p])
            if (c + 1) % GROUP == 0 or c == n_chunk - 1:
                image(from_inner, p, c - c % GROUP, c % GROUP + 1)

    def role_host(has_outer, cross, gets_far):
        gives_far = n_far if not has_outer and not cross else 0

        def send_up(c, p):
            far = gets_far and c < n_far
            bins = stack(c, p, False)
            if far:
                bins = [x + y for x, y in zip(bins, stack(c, p, True))]
            elif has_outer:
                await_bytes(from_outer.at[c, p], outer_recv.at[c, p])
            for t in range(NTAB):
                total = bins[t]
                if has_outer and not far:
                    total = total + from_outer[c, p, :, cols(t)].astype(jnp.float32)
                if cross:
                    own[c, p, :, cols(t)] = total
                up[c, p, :, cols(t)] = total.astype(jnp.bfloat16)
            up_copy(c, p, cross).start()

        def send_down(c, p):
            await_bytes(from_inner.at[c, p], inner_recv.at[c, p])
            for t in range(NTAB):
                total = own[c, p, :, cols(t)] + from_inner[c, p, :, cols(t)].astype(jnp.float32)
                down[c, p, :, cols(t)] = total.astype(jnp.bfloat16)
            if has_outer:
                down_copy(c, p).start()
            if p < pair - 1:
                client_copy(c, p).start()

        tasks = [(c, p) for c in range(n_chunk) for p in range(pair)]
        wait_masks(got_mask, mask_recv, 0)
        if gets_far:
            wait_masks(far_mask, far_mask_recv, 1)
        if cross:
            for i in range(len(tasks) + LAG):
                if i < len(tasks):
                    send_up(*tasks[i])
                if i >= LAG:
                    send_down(*tasks[i - LAG])
            table_load.wait()
            image(down, pair - 1, 0, n_chunk)
            wait_sends(True, 0)
            await_bytes(up, up_send)
            if has_outer:
                await_bytes(down, down_send)
            if pair > 1:
                await_bytes(down.at[:, pl.ds(0, pair - 1)], client_send)
        else:
            for c, p in tasks:
                if c >= gives_far:
                    send_up(c, p)
            wait_sends(True, gives_far)
            if gives_far < n_chunk:
                await_bytes(up.at[pl.ds(gives_far, n_chunk - gives_far)], up_send)
            finish(pair - 1)

    def role_client(p, far):
        wait_sends(False, far)
        finish(p)

    kinds = {}
    for d in range(n_det):
        kind = (0 < d < n_det - 1, d in (half - 1, half), n_far > 0 and d in (1, n_det - 2))
        kinds.setdefault(kind, []).append(d)
    for kind, members in kinds.items():
        here = functools.reduce(jnp.logical_or, [det == d for d in members])
        pl.when(here & is_host)(functools.partial(role_host, *kind))
        for p in range(pair - 1):
            far = 0 if kind[0] or kind[1] else n_far
            pl.when(here & (place(slab) == p))(functools.partial(role_client, p, far))


def body(n_slab, n_det, traces, tables, slab_range, table_slot, sample_start):
    _, frames, samp = traces.shape
    voxels = tables.shape[2]
    pair, n_chunk, n_far = sizes(n_slab, n_det, frames)
    n_tile = samp // LANES
    tiled = traces.reshape(frames // SUBLANES, SUBLANES, n_tile, LANES).transpose(0, 2, 1, 3)
    wide = NTAB * KWIN
    anywhere = pl.BlockSpec(memory_space=pl.ANY)
    dma = pltpu.SemaphoreType.DMA
    bf16, f32 = jnp.bfloat16, jnp.float32
    return pl.pallas_call(
        functools.partial(kernel, n_slab, n_det),
        out_shape=pltpu.VMEM((frames, voxels), f32),
        in_specs=[anywhere] * 5,
        out_specs=pl.BlockSpec(memory_space=pltpu.VMEM),
        scratch_shapes=[
            pltpu.VMEM((GROUPS, n_tile, SUBLANES, LANES), f32),
            pltpu.VMEM((frames // SUBLANES - GROUPS, n_tile, SUBLANES, LANES), f32),
            pltpu.VMEM(tables.shape, bf16),
            pltpu.SMEM(slab_range.shape, jnp.int32),
            pltpu.SMEM(table_slot.shape, jnp.int32),
            pltpu.SMEM(sample_start.shape, jnp.int32),
            pltpu.VMEM((OFFSETS, n_chunk, ROWS, KWIN), bf16),
            pltpu.VMEM((n_chunk, pair, OFFSETS, ROWS, KWIN), bf16),
            pltpu.VMEM((max(n_far, 1), pair, OFFSETS, ROWS, KWIN), bf16),
            pltpu.VMEM((OFFSETS, 1, LANES), f32),
            pltpu.VMEM((pair, OFFSETS, 1, LANES), f32),
            pltpu.VMEM((pair, OFFSETS, 1, LANES), f32),
            pltpu.VMEM((n_chunk, pair, ROWS, wide), f32),
            pltpu.VMEM((n_chunk, pair, ROWS, wide), bf16),
            pltpu.VMEM((n_chunk, pair, ROWS, wide), bf16),
            pltpu.VMEM((n_chunk, pair, ROWS, wide), bf16),
            pltpu.VMEM((n_chunk, pair, ROWS, wide), bf16),
            dma((2,)),
            dma,
            dma((3,)),
            dma,
            dma,
            dma((n_chunk, pair)),
            dma,
            dma((pair,)),
            dma,
            dma((pair,)),
            dma,
            dma((n_chunk, pair)),
            dma,
            dma,
            dma((n_chunk, pair)),
        ],
        compiler_params=pltpu.CompilerParams(
            collective_id=0, has_side_effects=True, vmem_limit_bytes=66_500_000
        ),
    )(tiled, tables, slab_range, table_slot, sample_start)


def solution(mesh):
    placed = (
        P(("slab", "det"), None, None),
        P("slab", None, "det"),
        P(("slab", "det"), None),
        P(("slab", "det"), None),
        P(("slab", "det"), None),
    )
    return jax.shard_map(
        functools.partial(body, mesh.shape["slab"], mesh.shape["det"]),
        mesh=mesh, in_specs=placed, out_specs=P(None, ("slab", "det")), check_vma=False,
    )
```

```python
import functools

import jax
import jax.numpy as jnp
from jax import lax
from jax.experimental import pallas as pl
from jax.experimental.pallas import tpu as pltpu
from jax.sharding import PartitionSpec as P

MESH = pl.DeviceIdType.MESH
KWIN = 256
NTAB = 4
RANGE = 3
LANES = 128
SUBLANES = 8
OFFSETS = 2 * RANGE + 1
ROWS = 16
LAG = 5
DIRECT = 2
SKIP = 0
AHEAD = 1
DOT = 32


def sizes(n_slab, n_det, frames):
    pair = 2 if n_slab % 2 == 0 else 1
    n_chunk = frames // ROWS
    far = range(SKIP, min(SKIP + DIRECT, n_chunk)) if n_det == 4 else range(0)
    return pair, n_chunk, far


def kernel(
    n_slab, n_det,
    traces, tables, slab_range, table_slot, sample_start, out,
    first_buf, rest_buf, table_buf, range_buf, slot_buf, start_buf,
    send_win, got_win, far_win, send_mask, got_mask, far_mask,
    own, up, from_outer, from_inner, down,
    trace_sem, table_sem, small_sem,
    win_send, far_send, win_recv, mask_send, mask_recv, far_mask_send, far_mask_recv,
    up_send, outer_recv, down_send, client_send, inner_recv,
):
    slab, det = lax.axis_index("slab"), lax.axis_index("det")
    frames = out.shape[0]
    pair, n_chunk, far_chunks = sizes(n_slab, n_det, frames)
    far_rows = len(far_chunks) * ROWS
    near_chunks = [c for c in range(n_chunk) if c not in far_chunks]
    order = [*far_chunks, *near_chunks]
    ahead = near_chunks[:AHEAD]
    edge_order = [*ahead, *far_chunks, *near_chunks[len(ahead) :]]
    half = n_det // 2

    edge = (det == 0) | (det == n_det - 1)

    def at_step(k):
        return k if edge_order[k] == order[k] else jnp.where(edge, edge_order[k], order[k])

    smalls = [
        pltpu.make_async_copy(src, dst, small_sem.at[i])
        for i, (src, dst) in enumerate(
            [(sample_start, start_buf), (slab_range, range_buf), (table_slot, slot_buf)]
        )
    ]
    for copy in smalls:
        copy.start()
    groups = ROWS // SUBLANES
    loads = [
        pltpu.make_async_copy(
            traces.at[pl.ds(at_step(0) * groups, groups)], first_buf, trace_sem.at[0]
        ),
        pltpu.make_async_copy(traces, rest_buf, trace_sem.at[1]),
    ]
    for copy in loads:
        copy.start()

    def valid(to):
        return (to >= 0) & (to < n_slab)

    def place(to):
        return lax.rem(to + pair * OFFSETS, pair)

    def hosts(to):
        return place(to) == pair - 1

    is_host = hosts(slab)
    host = slab - place(slab) + (pair - 1)
    left = det < half
    inner = jnp.where(left, det + 1, det - 1)
    outer = jnp.where(left, det - 1, det + 1)
    middle = (det == half - 1) | (det == half)

    def member(p):
        return host - (pair - 1) + p

    def sources(to):
        return jnp.minimum(to, RANGE) + jnp.minimum(n_slab - 1 - to, RANGE)

    source_counts = sorted({min(t, RANGE) + min(n_slab - 1 - t, RANGE) for t in range(n_slab)})

    def per_count(count, options, act):
        for n in options:
            pl.when(count == n)(functools.partial(act, n))

    barrier = pltpu.get_barrier_semaphore()
    heard = jnp.int32(0)

    def tell(condition, to, at):
        @pl.when(condition)
        def _():
            pl.semaphore_signal(barrier, 1, device_id=(to, at), device_id_type=MESH)

    for k in range(-RANGE, RANGE + pair):
        source, target = slab - k, slab + k
        writes = valid(target) & hosts(target)
        if k:
            tell(is_host & valid(source), source, det)
            heard = heard + writes.astype(jnp.int32)
        if far_rows:
            tell(is_host & middle & valid(source), source, outer)
            heard = heard + (writes & edge).astype(jnp.int32)
    if far_rows:
        tell(is_host & middle, slab, inner)
        heard = heard + (is_host & middle).astype(jnp.int32)
    else:
        for step in (-1, 1):
            near = det + step
            there = (near >= 0) & (near < n_det)
            for p in range(pair):
                tell(there & (is_host | (p == pair - 1)), member(p), near)
            heard = heard + jnp.where(there, jnp.where(is_host, pair, 1), 0)

    table_load = pltpu.make_async_copy(tables, table_buf, table_sem)
    table_load.start()

    for p in range(pair):
        for o in range(OFFSETS):

            @pl.when(is_host & jnp.logical_not(valid(member(p) - (o - RANGE))))
            def _():
                got_mask[p, o] = jnp.full(got_mask.shape[2:], -1, got_mask.dtype)
                far_mask[p, o] = jnp.full(far_mask.shape[2:], -1, far_mask.dtype)
                got_win[p, o] = jnp.zeros(got_win.shape[2:], got_win.dtype)
                far_win[p, o] = jnp.zeros(far_win.shape[2:], far_win.dtype)

    def send_copy(src, dst, to, at, sent, landed):
        return pltpu.make_async_remote_copy(
            src_ref=src, dst_ref=dst, send_sem=sent, recv_sem=landed,
            device_id=(to, at), device_id_type=MESH,
        )

    def await_bytes(ref, sem):
        pltpu.make_async_copy(ref, ref, sem).wait()

    def rows(c):
        return pl.ds(c * ROWS if isinstance(c, int) else pl.multiple_of(c * ROWS, ROWS), ROWS)

    def far_slot(c):
        return rows(c - far_chunks.start)

    def up_copy(c, p, cross):
        into, landed = (from_inner, inner_recv) if cross else (from_outer, outer_recv)
        return send_copy(up.at[p, rows(c)], into.at[p, rows(c)], slab, inner, up_send, landed.at[c, p])

    def down_copy(c, p):
        return send_copy(
            down.at[p, rows(c)], from_inner.at[p, rows(c)], member(p), outer, down_send, inner_recv.at[c, p]
        )

    def client_copy(c, p):
        return send_copy(
            down.at[p, rows(c)], from_inner.at[p, rows(c)], member(p), det, client_send, inner_recv.at[c, p]
        )

    for copy in smalls:
        copy.wait()
    n_tile = traces.shape[1]
    lane = lax.broadcasted_iota(jnp.int32, (SUBLANES, LANES), 1)
    firsts, backs, keeps = [], [], []
    for o in range(OFFSETS):
        target = slab + (o - RANGE)
        low, high, slot = (
            jnp.full(send_mask.shape[1:], value)
            for value in (range_buf[0, 0], range_buf[0, 1], slot_buf[0, o])
        )
        hit = (low <= target) & (target <= high)
        send_mask[o] = jnp.where(hit, slot, -1).astype(jnp.float32)
        start = start_buf[0, o]
        firsts.append(start >> 7)
        past = start & (LANES - 1)
        backs.append((LANES - past) & (LANES - 1))
        keeps.append(lane < LANES - past)

    def window(k, o):
        c = at_step(k)
        buf, base = (first_buf, 0) if k == 0 else (rest_buf, c * groups)
        for i in range(KWIN // LANES):
            pieces = []
            for g in range(groups):
                x, y = (
                    pltpu.roll(
                        buf[base + g, jnp.minimum(firsts[o] + i + n, n_tile - 1)], backs[o], 1
                    )
                    for n in range(2)
                )
                pieces.append(jnp.where(keeps[o], x, y))
            piece = jnp.concatenate(pieces, axis=0).astype(jnp.bfloat16)
            send_win[o, rows(c), i * LANES : (i + 1) * LANES] = piece

    def send(p, k=None):
        far = k is not None and edge_order[k] in far_chunks
        c = None if k is None else at_step(k)
        for o in range(OFFSETS):
            to = slab + (o - RANGE)
            at = to - p + (pair - 1)
            now = valid(to) & (place(to) == p)
            away = now & (at != slab)
            if c is None:
                src, near_dst, far_dst = send_mask.at[o], got_mask.at[p, o], far_mask.at[p, o]
                near_sems = mask_send, mask_recv.at[p]
                far_sems = far_mask_send, far_mask_recv.at[p]
            else:
                src, near_dst = send_win.at[o, rows(c)], got_win.at[p, o, rows(c)]
                near_sems = win_send, win_recv.at[c, p]
                if far:
                    far_dst = far_win.at[p, o, far_slot(edge_order[k])]
                    far_sems = far_send, outer_recv.at[edge_order[k], p]
            if far or (c is None and far_rows):
                pl.when(now & edge)(
                    lambda: send_copy(src, far_dst, at, inner, *far_sems).start()
                )
            pl.when(away & jnp.logical_not(edge) if far else away)(
                lambda: send_copy(src, near_dst, at, det, *near_sems).start()
            )

    for k in range(n_chunk):
        if k < len(loads):
            loads[k].wait()
        for o in range(OFFSETS):
            window(k, o)
        if k == 0:
            pl.semaphore_wait(barrier, heard)
            for p in range(pair):
                send(p)
        for p in range(pair):
            send(p, k)

    def stack(c, p, far):
        wins, masks, sem = (
            (far_win, far_mask, outer_recv) if far else (got_win, got_mask, win_recv)
        )

        slots = far_slot(c) if far else rows(c)

        def arrive(n):
            n = n + 1 if far else n
            if n:
                arrived = wins.at[p, pl.ds(0, n), slots]
                await_bytes(arrived, sem.at[c, p])

        per_count(sources(member(p)), source_counts, arrive)
        mine = None if far else RANGE - (pair - 1) + p
        bins = [jnp.zeros((ROWS, KWIN), jnp.float32) for _ in range(NTAB)]
        for o in range(OFFSETS):
            if o == mine:
                win, mask = send_win[o, rows(c)], send_mask[o]
            else:
                win, mask = wins[p, o, slots], masks[p, o]
            win = win.astype(jnp.float32)
            slot = jnp.broadcast_to(mask, (ROWS, LANES))
            slot = jnp.concatenate([slot] * (KWIN // LANES), axis=1)
            for t in range(NTAB):
                bins[t] = bins[t] + jnp.where(slot == t, win, 0.0)
        return bins

    def wait_masks(masks, sem, p, extra):
        def arrive(n):
            if n + extra:
                await_bytes(masks.at[p, pl.ds(0, n + extra)], sem.at[p])

        per_count(sources(member(p)), source_counts, arrive)

    def cols(t):
        return slice(t * KWIN, (t + 1) * KWIN)

    def image(ref, p, begin, end):
        weights = table_buf[...].reshape(NTAB * KWIN, table_buf.shape[2])
        out[begin:end] = jnp.dot(
            ref[p, begin:end], weights, preferred_element_type=jnp.float32
        )

    def wait_sends(hosting, far):
        local = pair if hosting else 0

        def sent(n):
            n = n + 1
            if n > local:
                if far < frames:
                    await_bytes(
                        send_win.at[pl.ds(0, n - local), pl.ds(0, frames - far)], win_send
                    )
                await_bytes(send_mask.at[pl.ds(0, n - local)], mask_send)
            if far:
                await_bytes(send_win.at[pl.ds(0, n), pl.ds(0, far)], far_send)
                await_bytes(send_mask.at[pl.ds(0, n)], far_mask_send)

        per_count(sources(slab), source_counts, sent)

    def finish(p):
        table_load.wait()
        group = []
        for c in order:
            if group and group[-1] + 1 != c:
                image(from_inner, p, group[0] * ROWS, (group[-1] + 1) * ROWS)
                group = []
            await_bytes(from_inner.at[p, rows(c)], inner_recv.at[c, p])
            group.append(c)
            if len(group) * ROWS >= DOT or c == order[-1]:
                image(from_inner, p, group[0] * ROWS, (group[-1] + 1) * ROWS)
                group = []

    def role_host(has_outer, cross, gets_far):
        gives = () if has_outer or cross else far_chunks

        def send_up(c, p):
            far = gets_far and c in far_chunks
            if c == order[0] or (gives and c == order[len(gives)]):
                wait_masks(got_mask, mask_recv, p, 0)
                if gets_far:
                    wait_masks(far_mask, far_mask_recv, p, 1)
            bins = stack(c, p, False)
            if far:
                bins = [x + y for x, y in zip(bins, stack(c, p, True))]
            elif has_outer:
                await_bytes(from_outer.at[p, rows(c)], outer_recv.at[c, p])
            for t in range(NTAB):
                total = bins[t]
                if has_outer and not far:
                    total = total + from_outer[p, rows(c), cols(t)].astype(jnp.float32)
                if cross:
                    own[p, rows(c), cols(t)] = total
                up[p, rows(c), cols(t)] = total.astype(jnp.bfloat16)
            up_copy(c, p, cross).start()

        def send_down(c, p):
            await_bytes(from_inner.at[p, rows(c)], inner_recv.at[c, p])
            for t in range(NTAB):
                total = own[p, rows(c), cols(t)] + from_inner[p, rows(c), cols(t)].astype(jnp.float32)
                down[p, rows(c), cols(t)] = total.astype(jnp.bfloat16)
            if has_outer:
                down_copy(c, p).start()
            if p < pair - 1:
                client_copy(c, p).start()

        tasks = [(c, p) for c in order for p in range(pair)]
        if cross:
            for i in range(len(tasks) + LAG):
                if i < len(tasks):
                    send_up(*tasks[i])
                if i >= LAG:
                    send_down(*tasks[i - LAG])
            table_load.wait()
            image(down, pair - 1, 0, frames)
            wait_sends(True, 0)
            await_bytes(up, up_send)
            if has_outer:
                await_bytes(down, down_send)
            if pair > 1:
                await_bytes(down.at[pl.ds(0, pair - 1)], client_send)
        else:
            for c, p in tasks:
                if c not in gives:
                    send_up(c, p)
            gone = len(gives) * ROWS
            wait_sends(True, gone)
            if gone < frames:
                await_bytes(up.at[:, pl.ds(0, frames - gone)], up_send)
            finish(pair - 1)

    def role_client(p, far):
        wait_sends(False, far)
        finish(p)

    kinds = {}
    for d in range(n_det):
        kind = (0 < d < n_det - 1, d in (half - 1, half), far_rows > 0 and d in (1, n_det - 2))
        kinds.setdefault(kind, []).append(d)
    for kind, members in kinds.items():
        here = functools.reduce(jnp.logical_or, [det == d for d in members])
        pl.when(here & is_host)(functools.partial(role_host, *kind))
        for p in range(pair - 1):
            far = 0 if kind[0] or kind[1] else far_rows
            pl.when(here & (place(slab) == p))(functools.partial(role_client, p, far))


def body(n_slab, n_det, traces, tables, slab_range, table_slot, sample_start):
    _, frames, samp = traces.shape
    voxels = tables.shape[2]
    pair, n_chunk, far_chunks = sizes(n_slab, n_det, frames)
    far_rows = max(len(far_chunks), 1) * ROWS
    head = ROWS // SUBLANES
    n_tile = samp // LANES
    tiled = traces.reshape(frames // SUBLANES, SUBLANES, n_tile, LANES).transpose(0, 2, 1, 3)
    wide = NTAB * KWIN
    anywhere = pl.BlockSpec(memory_space=pl.ANY)
    dma = pltpu.SemaphoreType.DMA
    bf16, f32 = jnp.bfloat16, jnp.float32
    return pl.pallas_call(
        functools.partial(kernel, n_slab, n_det),
        out_shape=pltpu.VMEM((frames, voxels), f32),
        in_specs=[anywhere] * 5,
        out_specs=pl.BlockSpec(memory_space=pltpu.VMEM),
        scratch_shapes=[
            pltpu.VMEM((head, n_tile, SUBLANES, LANES), f32),
            pltpu.VMEM((frames // SUBLANES, n_tile, SUBLANES, LANES), f32),
            pltpu.VMEM(tables.shape, bf16),
            pltpu.SMEM(slab_range.shape, jnp.int32),
            pltpu.SMEM(table_slot.shape, jnp.int32),
            pltpu.SMEM(sample_start.shape, jnp.int32),
            pltpu.VMEM((OFFSETS, frames, KWIN), bf16),
            pltpu.VMEM((pair, OFFSETS, frames, KWIN), bf16),
            pltpu.VMEM((pair, OFFSETS, far_rows, KWIN), bf16),
            pltpu.VMEM((OFFSETS, 1, LANES), f32),
            pltpu.VMEM((pair, OFFSETS, 1, LANES), f32),
            pltpu.VMEM((pair, OFFSETS, 1, LANES), f32),
            pltpu.VMEM((pair, frames, wide), f32),
            pltpu.VMEM((pair, frames, wide), bf16),
            pltpu.VMEM((pair, frames, wide), bf16),
            pltpu.VMEM((pair, frames, wide), bf16),
            pltpu.VMEM((pair, frames, wide), bf16),
            dma((2,)),
            dma,
            dma((3,)),
            dma,
            dma,
            dma((n_chunk, pair)),
            dma,
            dma((pair,)),
            dma,
            dma((pair,)),
            dma,
            dma((n_chunk, pair)),
            dma,
            dma,
            dma((n_chunk, pair)),
        ],
        compiler_params=pltpu.CompilerParams(
            collective_id=0, has_side_effects=True, vmem_limit_bytes=66_500_000
        ),
    )(tiled, tables, slab_range, table_slot, sample_start)


def solution(mesh):
    placed = (
        P(("slab", "det"), None, None),
        P("slab", None, "det"),
        P(("slab", "det"), None),
        P(("slab", "det"), None),
        P(("slab", "det"), None),
    )
    return jax.shard_map(
        functools.partial(body, mesh.shape["slab"], mesh.shape["det"]),
        mesh=mesh, in_specs=placed, out_specs=P(None, ("slab", "det")), check_vma=False,
    )
```

```python
import functools

import jax
import jax.numpy as jnp
from jax import lax
from jax.experimental import pallas as pl
from jax.experimental.pallas import tpu as pltpu
from jax.sharding import PartitionSpec as P

MESH = pl.DeviceIdType.MESH
KWIN = 256
NTAB = 4
RANGE = 3
LANES = 128
SUBLANES = 8
OFFSETS = 2 * RANGE + 1
ROWS = 16
LAG = 6
DIRECT = 2
SKIP = 0
AHEAD = 1
DOT = 32


def sizes(n_slab, n_det, frames):
    pair = 2 if n_slab % 2 == 0 else 1
    n_chunk = frames // ROWS
    far = range(SKIP, min(SKIP + DIRECT, n_chunk)) if n_det == 4 else range(0)
    return pair, n_chunk, far


def kernel(
    n_slab, n_det,
    traces, tables, slab_range, table_slot, sample_start, out,
    first_buf, next_buf, rest_buf, table_buf, range_buf, slot_buf, start_buf,
    send_win, got_win, far_win, send_mask, got_mask, far_mask,
    own, up, from_outer, from_inner, down,
    trace_sem, table_sem, small_sem,
    win_send, far_send, win_recv, mask_send, mask_recv, far_mask_send, far_mask_recv,
    up_send, outer_recv, down_send, client_send, inner_recv,
):
    slab, det = lax.axis_index("slab"), lax.axis_index("det")
    frames = out.shape[0]
    pair, n_chunk, far_chunks = sizes(n_slab, n_det, frames)
    far_rows = len(far_chunks) * ROWS
    near_chunks = [c for c in range(n_chunk) if c not in far_chunks]
    order = [*far_chunks, *near_chunks]
    ahead = near_chunks[:AHEAD]
    edge_order = [*ahead, *far_chunks, *near_chunks[len(ahead) :]]
    half = n_det // 2

    edge = (det == 0) | (det == n_det - 1)

    def at_step(k):
        return k if edge_order[k] == order[k] else jnp.where(edge, edge_order[k], order[k])

    smalls = [
        pltpu.make_async_copy(src, dst, small_sem.at[i])
        for i, (src, dst) in enumerate(
            [(sample_start, start_buf), (slab_range, range_buf), (table_slot, slot_buf)]
        )
    ]
    for copy in smalls:
        copy.start()
    groups = ROWS // SUBLANES
    loads = [
        pltpu.make_async_copy(
            traces.at[pl.ds(at_step(0) * groups, groups)], first_buf, trace_sem.at[0]
        ),
        pltpu.make_async_copy(
            traces.at[pl.ds(0, next_buf.shape[0])], next_buf, trace_sem.at[1]
        ),
        pltpu.make_async_copy(
            traces.at[pl.ds(next_buf.shape[0], rest_buf.shape[0])], rest_buf, trace_sem.at[2]
        ),
    ]
    for copy in loads:
        copy.start()

    def valid(to):
        return (to >= 0) & (to < n_slab)

    def place(to):
        return lax.rem(to + pair * OFFSETS, pair)

    def hosts(to):
        return place(to) == pair - 1

    is_host = hosts(slab)
    host = slab - place(slab) + (pair - 1)
    left = det < half
    inner = jnp.where(left, det + 1, det - 1)
    outer = jnp.where(left, det - 1, det + 1)
    middle = (det == half - 1) | (det == half)

    def member(p):
        return host - (pair - 1) + p

    def sources(to):
        return jnp.minimum(to, RANGE) + jnp.minimum(n_slab - 1 - to, RANGE)

    source_counts = sorted({min(t, RANGE) + min(n_slab - 1 - t, RANGE) for t in range(n_slab)})

    def per_count(count, options, act):
        for n in options:
            pl.when(count == n)(functools.partial(act, n))

    barrier = pltpu.get_barrier_semaphore()
    heard = jnp.int32(0)

    def tell(condition, to, at):
        @pl.when(condition)
        def _():
            pl.semaphore_signal(barrier, 1, device_id=(to, at), device_id_type=MESH)

    for k in range(-RANGE, RANGE + pair):
        source, target = slab - k, slab + k
        writes = valid(target) & hosts(target)
        if k:
            tell(is_host & valid(source), source, det)
            heard = heard + writes.astype(jnp.int32)
        if far_rows:
            tell(is_host & middle & valid(source), source, outer)
            heard = heard + (writes & edge).astype(jnp.int32)
    if far_rows:
        tell(is_host & middle, slab, inner)
        heard = heard + (is_host & middle).astype(jnp.int32)
    else:
        for step in (-1, 1):
            near = det + step
            there = (near >= 0) & (near < n_det)
            for p in range(pair):
                tell(there & (is_host | (p == pair - 1)), member(p), near)
            heard = heard + jnp.where(there, jnp.where(is_host, pair, 1), 0)

    table_load = pltpu.make_async_copy(tables, table_buf, table_sem)

    for p in range(pair):
        for o in range(OFFSETS):

            @pl.when(is_host & jnp.logical_not(valid(member(p) - (o - RANGE))))
            def _():
                got_mask[p, o] = jnp.full(got_mask.shape[2:], -1, got_mask.dtype)
                far_mask[p, o] = jnp.full(far_mask.shape[2:], -1, far_mask.dtype)
                got_win[p, o] = jnp.zeros(got_win.shape[2:], got_win.dtype)
                far_win[p, o] = jnp.zeros(far_win.shape[2:], far_win.dtype)

    def send_copy(src, dst, to, at, sent, landed):
        return pltpu.make_async_remote_copy(
            src_ref=src, dst_ref=dst, send_sem=sent, recv_sem=landed,
            device_id=(to, at), device_id_type=MESH,
        )

    def await_bytes(ref, sem):
        pltpu.make_async_copy(ref, ref, sem).wait()

    def rows(c):
        return pl.ds(c * ROWS if isinstance(c, int) else pl.multiple_of(c * ROWS, ROWS), ROWS)

    def far_slot(c):
        return rows(c - far_chunks.start)

    def up_copy(c, p, cross):
        into, landed = (from_inner, inner_recv) if cross else (from_outer, outer_recv)
        return send_copy(up.at[p, rows(c)], into.at[p, rows(c)], slab, inner, up_send, landed.at[c, p])

    def down_copy(c, p):
        return send_copy(
            down.at[p, rows(c)], from_inner.at[p, rows(c)], member(p), outer, down_send, inner_recv.at[c, p]
        )

    def client_copy(c, p):
        return send_copy(
            down.at[p, rows(c)], from_inner.at[p, rows(c)], member(p), det, client_send, inner_recv.at[c, p]
        )

    for copy in smalls:
        copy.wait()
    n_tile = traces.shape[1]
    lane = lax.broadcasted_iota(jnp.int32, (SUBLANES, LANES), 1)
    firsts, backs, keeps = [], [], []
    for o in range(OFFSETS):
        target = slab + (o - RANGE)
        low, high, slot = (
            jnp.full(send_mask.shape[1:], value)
            for value in (range_buf[0, 0], range_buf[0, 1], slot_buf[0, o])
        )
        hit = (low <= target) & (target <= high)
        send_mask[o] = jnp.where(hit, slot, -1).astype(jnp.float32)
        start = start_buf[0, o]
        firsts.append(start >> 7)
        past = start & (LANES - 1)
        backs.append((LANES - past) & (LANES - 1))
        keeps.append(lane < LANES - past)

    def window(k, o):
        c = at_step(k)
        buf, base = first_buf, 0
        if k:
            early = max(edge_order[k], order[k]) < next_buf.shape[0] // groups
            buf, base = (next_buf, c * groups) if early else (rest_buf, c * groups - next_buf.shape[0])
        for i in range(KWIN // LANES):
            pieces = []
            for g in range(groups):
                x, y = (
                    pltpu.roll(
                        buf[base + g, jnp.minimum(firsts[o] + i + n, n_tile - 1)], backs[o], 1
                    )
                    for n in range(2)
                )
                pieces.append(jnp.where(keeps[o], x, y))
            piece = jnp.concatenate(pieces, axis=0).astype(jnp.bfloat16)
            send_win[o, rows(c), i * LANES : (i + 1) * LANES] = piece

    def send(p, k=None):
        far = k is not None and edge_order[k] in far_chunks
        c = None if k is None else at_step(k)
        for o in range(OFFSETS):
            to = slab + (o - RANGE)
            at = to - p + (pair - 1)
            now = valid(to) & (place(to) == p)
            away = now & (at != slab)
            if c is None:
                src, near_dst, far_dst = send_mask.at[o], got_mask.at[p, o], far_mask.at[p, o]
                near_sems = mask_send, mask_recv.at[p]
                far_sems = far_mask_send, far_mask_recv.at[p]
            else:
                src, near_dst = send_win.at[o, rows(c)], got_win.at[p, o, rows(c)]
                near_sems = win_send, win_recv.at[c, p]
                if far:
                    far_dst = far_win.at[p, o, far_slot(edge_order[k])]
                    far_sems = far_send, outer_recv.at[edge_order[k], p]
            if far or (c is None and far_rows):
                pl.when(now & edge)(
                    lambda: send_copy(src, far_dst, at, inner, *far_sems).start()
                )
            pl.when(away & jnp.logical_not(edge) if far else away)(
                lambda: send_copy(src, near_dst, at, det, *near_sems).start()
            )

    for k in range(n_chunk):
        if k < 2:
            loads[k].wait()
        if k * groups == next_buf.shape[0]:
            loads[2].wait()
        for o in range(OFFSETS):
            window(k, o)
        if k == 0:
            pl.semaphore_wait(barrier, heard)
            for p in range(pair):
                send(p)
        for p in range(pair):
            send(p, k)

    table_load.start()

    def stack(c, p, far):
        wins, masks, sem = (
            (far_win, far_mask, outer_recv) if far else (got_win, got_mask, win_recv)
        )

        slots = far_slot(c) if far else rows(c)

        def arrive(n):
            n = n + 1 if far else n
            if n:
                arrived = wins.at[p, pl.ds(0, n), slots]
                await_bytes(arrived, sem.at[c, p])

        per_count(sources(member(p)), source_counts, arrive)
        mine = None if far else RANGE - (pair - 1) + p
        bins = [jnp.zeros((ROWS, KWIN), jnp.float32) for _ in range(NTAB)]
        for o in range(OFFSETS):
            if o == mine:
                win, mask = send_win[o, rows(c)], send_mask[o]
            else:
                win, mask = wins[p, o, slots], masks[p, o]
            win = win.astype(jnp.float32)
            slot = jnp.broadcast_to(mask, (ROWS, LANES))
            slot = jnp.concatenate([slot] * (KWIN // LANES), axis=1)
            for t in range(NTAB):
                bins[t] = bins[t] + jnp.where(slot == t, win, 0.0)
        return bins

    def wait_masks(masks, sem, p, extra):
        def arrive(n):
            if n + extra:
                await_bytes(masks.at[p, pl.ds(0, n + extra)], sem.at[p])

        per_count(sources(member(p)), source_counts, arrive)

    def cols(t):
        return slice(t * KWIN, (t + 1) * KWIN)

    def image(ref, p, begin, end):
        weights = table_buf[...].reshape(NTAB * KWIN, table_buf.shape[2])
        out[begin:end] = jnp.dot(
            ref[p, begin:end], weights, preferred_element_type=jnp.float32
        )

    def wait_sends(hosting, far):
        local = pair if hosting else 0

        def sent(n):
            n = n + 1
            if n > local:
                if far < frames:
                    await_bytes(
                        send_win.at[pl.ds(0, n - local), pl.ds(0, frames - far)], win_send
                    )
                await_bytes(send_mask.at[pl.ds(0, n - local)], mask_send)
            if far:
                await_bytes(send_win.at[pl.ds(0, n), pl.ds(0, far)], far_send)
                await_bytes(send_mask.at[pl.ds(0, n)], far_mask_send)

        per_count(sources(slab), source_counts, sent)

    def finish(p):
        table_load.wait()
        group = []
        for c in order:
            if group and group[-1] + 1 != c:
                image(from_inner, p, group[0] * ROWS, (group[-1] + 1) * ROWS)
                group = []
            await_bytes(from_inner.at[p, rows(c)], inner_recv.at[c, p])
            group.append(c)
            if len(group) * ROWS >= DOT or c == order[-1]:
                image(from_inner, p, group[0] * ROWS, (group[-1] + 1) * ROWS)
                group = []

    def role_host(has_outer, cross, gets_far):
        gives = () if has_outer or cross else far_chunks

        def send_up(c, p):
            far = gets_far and c in far_chunks
            if c == order[0] or (gives and c == order[len(gives)]):
                wait_masks(got_mask, mask_recv, p, 0)
                if gets_far:
                    wait_masks(far_mask, far_mask_recv, p, 1)
            bins = stack(c, p, False)
            if far:
                bins = [x + y for x, y in zip(bins, stack(c, p, True))]
            elif has_outer:
                await_bytes(from_outer.at[p, rows(c)], outer_recv.at[c, p])
            for t in range(NTAB):
                total = bins[t]
                if has_outer and not far:
                    total = total + from_outer[p, rows(c), cols(t)].astype(jnp.float32)
                if cross:
                    own[p, rows(c), cols(t)] = total
                up[p, rows(c), cols(t)] = total.astype(jnp.bfloat16)
            up_copy(c, p, cross).start()

        def send_down(c, p):
            await_bytes(from_inner.at[p, rows(c)], inner_recv.at[c, p])
            for t in range(NTAB):
                total = own[p, rows(c), cols(t)] + from_inner[p, rows(c), cols(t)].astype(jnp.float32)
                down[p, rows(c), cols(t)] = total.astype(jnp.bfloat16)
            if has_outer:
                down_copy(c, p).start()
            if p < pair - 1:
                client_copy(c, p).start()

        tasks = [(c, p) for c in order for p in range(pair)]
        if cross:
            for i in range(len(tasks) + LAG):
                if i < len(tasks):
                    send_up(*tasks[i])
                if i >= LAG:
                    send_down(*tasks[i - LAG])
            table_load.wait()
            image(down, pair - 1, 0, frames)
            wait_sends(True, 0)
            await_bytes(up, up_send)
            if has_outer:
                await_bytes(down, down_send)
            if pair > 1:
                await_bytes(down.at[pl.ds(0, pair - 1)], client_send)
        else:
            for c, p in tasks:
                if c not in gives:
                    send_up(c, p)
            gone = len(gives) * ROWS
            wait_sends(True, gone)
            if gone < frames:
                await_bytes(up.at[:, pl.ds(0, frames - gone)], up_send)
            finish(pair - 1)

    def role_client(p, far):
        wait_sends(False, far)
        finish(p)

    kinds = {}
    for d in range(n_det):
        kind = (0 < d < n_det - 1, d in (half - 1, half), far_rows > 0 and d in (1, n_det - 2))
        kinds.setdefault(kind, []).append(d)
    for kind, members in kinds.items():
        here = functools.reduce(jnp.logical_or, [det == d for d in members])
        pl.when(here & is_host)(functools.partial(role_host, *kind))
        for p in range(pair - 1):
            far = 0 if kind[0] or kind[1] else far_rows
            pl.when(here & (place(slab) == p))(functools.partial(role_client, p, far))


def body(n_slab, n_det, traces, tables, slab_range, table_slot, sample_start):
    _, frames, samp = traces.shape
    voxels = tables.shape[2]
    pair, n_chunk, far_chunks = sizes(n_slab, n_det, frames)
    far_rows = max(len(far_chunks), 1) * ROWS
    head = ROWS // SUBLANES
    soon = len(far_chunks) + AHEAD
    n_tile = samp // LANES
    tiled = traces.reshape(frames // SUBLANES, SUBLANES, n_tile, LANES).transpose(0, 2, 1, 3)
    wide = NTAB * KWIN
    anywhere = pl.BlockSpec(memory_space=pl.ANY)
    dma = pltpu.SemaphoreType.DMA
    bf16, f32 = jnp.bfloat16, jnp.float32
    return pl.pallas_call(
        functools.partial(kernel, n_slab, n_det),
        out_shape=pltpu.VMEM((frames, voxels), f32),
        in_specs=[anywhere] * 5,
        out_specs=pl.BlockSpec(memory_space=pltpu.VMEM),
        scratch_shapes=[
            pltpu.VMEM((head, n_tile, SUBLANES, LANES), f32),
            pltpu.VMEM((soon * head, n_tile, SUBLANES, LANES), f32),
            pltpu.VMEM((frames // SUBLANES - soon * head, n_tile, SUBLANES, LANES), f32),
            pltpu.VMEM(tables.shape, bf16),
            pltpu.SMEM(slab_range.shape, jnp.int32),
            pltpu.SMEM(table_slot.shape, jnp.int32),
            pltpu.SMEM(sample_start.shape, jnp.int32),
            pltpu.VMEM((OFFSETS, frames, KWIN), bf16),
            pltpu.VMEM((pair, OFFSETS, frames, KWIN), bf16),
            pltpu.VMEM((pair, OFFSETS, far_rows, KWIN), bf16),
            pltpu.VMEM((OFFSETS, 1, LANES), f32),
            pltpu.VMEM((pair, OFFSETS, 1, LANES), f32),
            pltpu.VMEM((pair, OFFSETS, 1, LANES), f32),
            pltpu.VMEM((pair, frames, wide), f32),
            pltpu.VMEM((pair, frames, wide), bf16),
            pltpu.VMEM((pair, frames, wide), bf16),
            pltpu.VMEM((pair, frames, wide), bf16),
            pltpu.VMEM((pair, frames, wide), bf16),
            dma((3,)),
            dma,
            dma((3,)),
            dma,
            dma,
            dma((n_chunk, pair)),
            dma,
            dma((pair,)),
            dma,
            dma((pair,)),
            dma,
            dma((n_chunk, pair)),
            dma,
            dma,
            dma((n_chunk, pair)),
        ],
        compiler_params=pltpu.CompilerParams(
            collective_id=0, has_side_effects=True, vmem_limit_bytes=66_500_000
        ),
    )(tiled, tables, slab_range, table_slot, sample_start)


def solution(mesh):
    placed = (
        P(("slab", "det"), None, None),
        P("slab", None, "det"),
        P(("slab", "det"), None),
        P(("slab", "det"), None),
        P(("slab", "det"), None),
    )
    return jax.shard_map(
        functools.partial(body, mesh.shape["slab"], mesh.shape["det"]),
        mesh=mesh, in_specs=placed, out_specs=P(None, ("slab", "det")), check_vma=False,
    )
```

```python
import functools

import jax
import jax.numpy as jnp
from jax import lax
from jax.experimental import pallas as pl
from jax.experimental.pallas import tpu as pltpu
from jax.sharding import PartitionSpec as P

MESH = pl.DeviceIdType.MESH
KWIN = 256
NTAB = 4
RANGE = 3
LANES = 128
SUBLANES = 8
OFFSETS = 2 * RANGE + 1
ROWS = 16
LAG = 6
DIRECT = 2
SKIP = 0
AHEAD = 1
TAIL = 2
DOT = 16


def sizes(n_slab, n_det, frames):
    pair = 2 if n_slab % 2 == 0 else 1
    n_chunk = frames // ROWS
    far = range(SKIP, min(SKIP + DIRECT, n_chunk)) if n_det == 4 else range(0)
    return pair, n_chunk, far


def kernel(
    n_slab, n_det,
    traces, tables, slab_range, table_slot, sample_start, out,
    first_buf, next_buf, rest_buf, table_buf, range_buf, slot_buf, start_buf,
    send_win, got_win, far_win, send_mask, got_mask, far_mask,
    own, up, from_outer, from_inner, down,
    trace_sem, table_sem, small_sem,
    win_send, far_send, win_recv, mask_send, mask_recv, far_mask_send, far_mask_recv,
    up_send, outer_recv, down_send, client_send, inner_recv,
):
    slab, det = lax.axis_index("slab"), lax.axis_index("det")
    frames = out.shape[0]
    pair, n_chunk, far_chunks = sizes(n_slab, n_det, frames)
    far_rows = len(far_chunks) * ROWS
    near_chunks = [c for c in range(n_chunk) if c not in far_chunks]
    order = [*far_chunks, *near_chunks]
    ahead = near_chunks[:AHEAD]
    edge_order = [*ahead, *far_chunks, *near_chunks[len(ahead) :]]
    half = n_det // 2

    edge = (det == 0) | (det == n_det - 1)

    def at_step(k):
        return k if edge_order[k] == order[k] else jnp.where(edge, edge_order[k], order[k])

    smalls = [
        pltpu.make_async_copy(src, dst, small_sem.at[i])
        for i, (src, dst) in enumerate(
            [(sample_start, start_buf), (slab_range, range_buf), (table_slot, slot_buf)]
        )
    ]
    for copy in smalls:
        copy.start()
    groups = ROWS // SUBLANES
    loads = [
        pltpu.make_async_copy(
            traces.at[pl.ds(at_step(0) * groups, groups)], first_buf, trace_sem.at[0]
        ),
        pltpu.make_async_copy(
            traces.at[pl.ds(0, next_buf.shape[0])], next_buf, trace_sem.at[1]
        ),
        pltpu.make_async_copy(
            traces.at[pl.ds(next_buf.shape[0], rest_buf.shape[0])], rest_buf, trace_sem.at[2]
        ),
    ]
    for copy in loads:
        copy.start()

    def valid(to):
        return (to >= 0) & (to < n_slab)

    def place(to):
        return lax.rem(to + pair * OFFSETS, pair)

    def hosts(to):
        return place(to) == pair - 1

    is_host = hosts(slab)
    host = slab - place(slab) + (pair - 1)
    left = det < half
    inner = jnp.where(left, det + 1, det - 1)
    outer = jnp.where(left, det - 1, det + 1)
    middle = (det == half - 1) | (det == half)

    def member(p):
        return host - (pair - 1) + p

    def sources(to):
        return jnp.minimum(to, RANGE) + jnp.minimum(n_slab - 1 - to, RANGE)

    source_counts = sorted({min(t, RANGE) + min(n_slab - 1 - t, RANGE) for t in range(n_slab)})

    def per_count(count, options, act):
        for n in options:
            pl.when(count == n)(functools.partial(act, n))

    barrier = pltpu.get_barrier_semaphore()
    heard = jnp.int32(0)

    def tell(condition, to, at):
        @pl.when(condition)
        def _():
            pl.semaphore_signal(barrier, 1, device_id=(to, at), device_id_type=MESH)

    for k in range(-RANGE, RANGE + pair):
        source, target = slab - k, slab + k
        writes = valid(target) & hosts(target)
        if k:
            tell(is_host & valid(source), source, det)
            heard = heard + writes.astype(jnp.int32)
        if far_rows:
            tell(is_host & middle & valid(source), source, outer)
            heard = heard + (writes & edge).astype(jnp.int32)
    if far_rows:
        tell(is_host & middle, slab, inner)
        heard = heard + (is_host & middle).astype(jnp.int32)
    else:
        for step in (-1, 1):
            near = det + step
            there = (near >= 0) & (near < n_det)
            for p in range(pair):
                tell(there & (is_host | (p == pair - 1)), member(p), near)
            heard = heard + jnp.where(there, jnp.where(is_host, pair, 1), 0)

    table_load = pltpu.make_async_copy(tables, table_buf, table_sem)

    for p in range(pair):
        for o in range(OFFSETS):

            @pl.when(is_host & jnp.logical_not(valid(member(p) - (o - RANGE))))
            def _():
                got_mask[p, o] = jnp.full(got_mask.shape[2:], -1, got_mask.dtype)
                far_mask[p, o] = jnp.full(far_mask.shape[2:], -1, far_mask.dtype)
                got_win[p, o] = jnp.zeros(got_win.shape[2:], got_win.dtype)
                far_win[p, o] = jnp.zeros(far_win.shape[2:], far_win.dtype)

    def send_copy(src, dst, to, at, sent, landed):
        return pltpu.make_async_remote_copy(
            src_ref=src, dst_ref=dst, send_sem=sent, recv_sem=landed,
            device_id=(to, at), device_id_type=MESH,
        )

    def await_bytes(ref, sem):
        pltpu.make_async_copy(ref, ref, sem).wait()

    def rows(c):
        return pl.ds(c * ROWS if isinstance(c, int) else pl.multiple_of(c * ROWS, ROWS), ROWS)

    def far_slot(c):
        return rows(c - far_chunks.start)

    def up_copy(c, p, cross):
        into, landed = (from_inner, inner_recv) if cross else (from_outer, outer_recv)
        return send_copy(up.at[p, rows(c)], into.at[p, rows(c)], slab, inner, up_send, landed.at[c, p])

    def down_copy(c, p):
        return send_copy(
            down.at[p, rows(c)], from_inner.at[p, rows(c)], member(p), outer, down_send, inner_recv.at[c, p]
        )

    def client_copy(c, p):
        return send_copy(
            down.at[p, rows(c)], from_inner.at[p, rows(c)], member(p), det, client_send, inner_recv.at[c, p]
        )

    for copy in smalls:
        copy.wait()
    n_tile = traces.shape[1]
    lane = lax.broadcasted_iota(jnp.int32, (SUBLANES, LANES), 1)
    firsts, backs, keeps = [], [], []
    for o in range(OFFSETS):
        target = slab + (o - RANGE)
        low, high, slot = (
            jnp.full(send_mask.shape[1:], value)
            for value in (range_buf[0, 0], range_buf[0, 1], slot_buf[0, o])
        )
        hit = (low <= target) & (target <= high)
        send_mask[o] = jnp.where(hit, slot, -1).astype(jnp.float32)
        start = start_buf[0, o]
        firsts.append(start >> 7)
        past = start & (LANES - 1)
        backs.append((LANES - past) & (LANES - 1))
        keeps.append(lane < LANES - past)

    def window(k, o):
        c = at_step(k)
        buf, base = first_buf, 0
        if k:
            early = max(edge_order[k], order[k]) < next_buf.shape[0] // groups
            buf, base = (next_buf, c * groups) if early else (rest_buf, c * groups - next_buf.shape[0])
        for i in range(KWIN // LANES):
            pieces = []
            for g in range(groups):
                x, y = (
                    pltpu.roll(
                        buf[base + g, jnp.minimum(firsts[o] + i + n, n_tile - 1)], backs[o], 1
                    )
                    for n in range(2)
                )
                pieces.append(jnp.where(keeps[o], x, y))
            piece = jnp.concatenate(pieces, axis=0).astype(jnp.bfloat16)
            send_win[o, rows(c), i * LANES : (i + 1) * LANES] = piece

    def send(p, k=None):
        far = k is not None and edge_order[k] in far_chunks
        c = None if k is None else at_step(k)
        for o in range(OFFSETS):
            to = slab + (o - RANGE)
            at = to - p + (pair - 1)
            now = valid(to) & (place(to) == p)
            away = now & (at != slab)
            if c is None:
                src, near_dst, far_dst = send_mask.at[o], got_mask.at[p, o], far_mask.at[p, o]
                near_sems = mask_send, mask_recv.at[p]
                far_sems = far_mask_send, far_mask_recv.at[p]
            else:
                src, near_dst = send_win.at[o, rows(c)], got_win.at[p, o, rows(c)]
                near_sems = win_send, win_recv.at[c, p]
                if far:
                    far_dst = far_win.at[p, o, far_slot(edge_order[k])]
                    far_sems = far_send, outer_recv.at[edge_order[k], p]
            if far or (c is None and far_rows):
                pl.when(now & edge)(
                    lambda: send_copy(src, far_dst, at, inner, *far_sems).start()
                )
            pl.when(away & jnp.logical_not(edge) if far else away)(
                lambda: send_copy(src, near_dst, at, det, *near_sems).start()
            )

    for k in range(n_chunk):
        if k < 2:
            loads[k].wait()
        if k * groups == next_buf.shape[0]:
            loads[2].wait()
        for o in range(OFFSETS):
            window(k, o)
        if k == 0:
            pl.semaphore_wait(barrier, heard)
            for p in range(pair):
                send(p)
        for p in range(pair):
            send(p, k)

    table_load.start()

    def stack(c, p, far):
        wins, masks, sem = (
            (far_win, far_mask, outer_recv) if far else (got_win, got_mask, win_recv)
        )

        slots = far_slot(c) if far else rows(c)

        def arrive(n):
            n = n + 1 if far else n
            if n:
                arrived = wins.at[p, pl.ds(0, n), slots]
                await_bytes(arrived, sem.at[c, p])

        per_count(sources(member(p)), source_counts, arrive)
        mine = None if far else RANGE - (pair - 1) + p
        bins = [jnp.zeros((ROWS, KWIN), jnp.float32) for _ in range(NTAB)]
        for o in range(OFFSETS):
            if o == mine:
                win, mask = send_win[o, rows(c)], send_mask[o]
            else:
                win, mask = wins[p, o, slots], masks[p, o]
            win = win.astype(jnp.float32)
            slot = jnp.broadcast_to(mask, (ROWS, LANES))
            slot = jnp.concatenate([slot] * (KWIN // LANES), axis=1)
            for t in range(NTAB):
                bins[t] = bins[t] + jnp.where(slot == t, win, 0.0)
        return bins

    def wait_masks(masks, sem, p, extra):
        def arrive(n):
            if n + extra:
                await_bytes(masks.at[p, pl.ds(0, n + extra)], sem.at[p])

        per_count(sources(member(p)), source_counts, arrive)

    def cols(t):
        return slice(t * KWIN, (t + 1) * KWIN)

    def image(ref, p, begin, end):
        weights = table_buf[...].reshape(NTAB * KWIN, table_buf.shape[2])
        out[begin:end] = jnp.dot(
            ref[p, begin:end], weights, preferred_element_type=jnp.float32
        )

    def wait_sends(hosting, far):
        local = pair if hosting else 0

        def sent(n):
            n = n + 1
            if n > local:
                if far < frames:
                    await_bytes(
                        send_win.at[pl.ds(0, n - local), pl.ds(0, frames - far)], win_send
                    )
                await_bytes(send_mask.at[pl.ds(0, n - local)], mask_send)
            if far:
                await_bytes(send_win.at[pl.ds(0, n), pl.ds(0, far)], far_send)
                await_bytes(send_mask.at[pl.ds(0, n)], far_mask_send)

        per_count(sources(slab), source_counts, sent)

    def finish(p):
        table_load.wait()
        group = []
        for c in order:
            if group and group[-1] + 1 != c:
                image(from_inner, p, group[0] * ROWS, (group[-1] + 1) * ROWS)
                group = []
            await_bytes(from_inner.at[p, rows(c)], inner_recv.at[c, p])
            group.append(c)
            if len(group) * ROWS >= DOT or c == order[-1]:
                image(from_inner, p, group[0] * ROWS, (group[-1] + 1) * ROWS)
                group = []

    def role_host(has_outer, cross, gets_far):
        gives = () if has_outer or cross else far_chunks

        def send_up(c, p):
            far = gets_far and c in far_chunks
            if c == order[0] or (gives and c == order[len(gives)]):
                wait_masks(got_mask, mask_recv, p, 0)
                if gets_far:
                    wait_masks(far_mask, far_mask_recv, p, 1)
            bins = stack(c, p, False)
            if far:
                bins = [x + y for x, y in zip(bins, stack(c, p, True))]
            elif has_outer:
                await_bytes(from_outer.at[p, rows(c)], outer_recv.at[c, p])
            for t in range(NTAB):
                total = bins[t]
                if has_outer and not far:
                    total = total + from_outer[p, rows(c), cols(t)].astype(jnp.float32)
                if cross:
                    own[p, rows(c), cols(t)] = total
                up[p, rows(c), cols(t)] = total.astype(jnp.bfloat16)
            up_copy(c, p, cross).start()

        def send_down(c, p):
            await_bytes(from_inner.at[p, rows(c)], inner_recv.at[c, p])
            for t in range(NTAB):
                total = own[p, rows(c), cols(t)] + from_inner[p, rows(c), cols(t)].astype(jnp.float32)
                down[p, rows(c), cols(t)] = total.astype(jnp.bfloat16)
            if has_outer:
                down_copy(c, p).start()
            if p < pair - 1:
                client_copy(c, p).start()

        tasks = [(c, p) for c in order[:-TAIL] for p in range(pair)]
        tasks += [(c, p) for p in range(pair) for c in order[-TAIL:]]
        if cross:
            for i in range(len(tasks) + LAG):
                if i < len(tasks):
                    send_up(*tasks[i])
                if i >= LAG:
                    send_down(*tasks[i - LAG])
            table_load.wait()
            image(down, pair - 1, 0, frames)
            wait_sends(True, 0)
            await_bytes(up, up_send)
            if has_outer:
                await_bytes(down, down_send)
            if pair > 1:
                await_bytes(down.at[pl.ds(0, pair - 1)], client_send)
        else:
            for c, p in tasks:
                if c not in gives:
                    send_up(c, p)
            gone = len(gives) * ROWS
            wait_sends(True, gone)
            if gone < frames:
                await_bytes(up.at[:, pl.ds(0, frames - gone)], up_send)
            finish(pair - 1)

    def role_client(p, far):
        wait_sends(False, far)
        finish(p)

    kinds = {}
    for d in range(n_det):
        kind = (0 < d < n_det - 1, d in (half - 1, half), far_rows > 0 and d in (1, n_det - 2))
        kinds.setdefault(kind, []).append(d)
    for kind, members in kinds.items():
        here = functools.reduce(jnp.logical_or, [det == d for d in members])
        pl.when(here & is_host)(functools.partial(role_host, *kind))
        for p in range(pair - 1):
            far = 0 if kind[0] or kind[1] else far_rows
            pl.when(here & (place(slab) == p))(functools.partial(role_client, p, far))


def body(n_slab, n_det, traces, tables, slab_range, table_slot, sample_start):
    _, frames, samp = traces.shape
    voxels = tables.shape[2]
    pair, n_chunk, far_chunks = sizes(n_slab, n_det, frames)
    far_rows = max(len(far_chunks), 1) * ROWS
    head = ROWS // SUBLANES
    soon = len(far_chunks) + AHEAD
    n_tile = samp // LANES
    tiled = traces.reshape(frames // SUBLANES, SUBLANES, n_tile, LANES).transpose(0, 2, 1, 3)
    wide = NTAB * KWIN
    anywhere = pl.BlockSpec(memory_space=pl.ANY)
    dma = pltpu.SemaphoreType.DMA
    bf16, f32 = jnp.bfloat16, jnp.float32
    return pl.pallas_call(
        functools.partial(kernel, n_slab, n_det),
        out_shape=pltpu.VMEM((frames, voxels), f32),
        in_specs=[anywhere] * 5,
        out_specs=pl.BlockSpec(memory_space=pltpu.VMEM),
        scratch_shapes=[
            pltpu.VMEM((head, n_tile, SUBLANES, LANES), f32),
            pltpu.VMEM((soon * head, n_tile, SUBLANES, LANES), f32),
            pltpu.VMEM((frames // SUBLANES - soon * head, n_tile, SUBLANES, LANES), f32),
            pltpu.VMEM(tables.shape, bf16),
            pltpu.SMEM(slab_range.shape, jnp.int32),
            pltpu.SMEM(table_slot.shape, jnp.int32),
            pltpu.SMEM(sample_start.shape, jnp.int32),
            pltpu.VMEM((OFFSETS, frames, KWIN), bf16),
            pltpu.VMEM((pair, OFFSETS, frames, KWIN), bf16),
            pltpu.VMEM((pair, OFFSETS, far_rows, KWIN), bf16),
            pltpu.VMEM((OFFSETS, 1, LANES), f32),
            pltpu.VMEM((pair, OFFSETS, 1, LANES), f32),
            pltpu.VMEM((pair, OFFSETS, 1, LANES), f32),
            pltpu.VMEM((pair, frames, wide), f32),
            pltpu.VMEM((pair, frames, wide), bf16),
            pltpu.VMEM((pair, frames, wide), bf16),
            pltpu.VMEM((pair, frames, wide), bf16),
            pltpu.VMEM((pair, frames, wide), bf16),
            dma((3,)),
            dma,
            dma((3,)),
            dma,
            dma,
            dma((n_chunk, pair)),
            dma,
            dma((pair,)),
            dma,
            dma((pair,)),
            dma,
            dma((n_chunk, pair)),
            dma,
            dma,
            dma((n_chunk, pair)),
        ],
        compiler_params=pltpu.CompilerParams(
            collective_id=0, has_side_effects=True, vmem_limit_bytes=66_500_000
        ),
    )(tiled, tables, slab_range, table_slot, sample_start)


def solution(mesh):
    placed = (
        P(("slab", "det"), None, None),
        P("slab", None, "det"),
        P(("slab", "det"), None),
        P(("slab", "det"), None),
        P(("slab", "det"), None),
    )
    return jax.shard_map(
        functools.partial(body, mesh.shape["slab"], mesh.shape["det"]),
        mesh=mesh, in_specs=placed, out_specs=P(None, ("slab", "det")), check_vma=False,
    )
```
